128 devices in a mesh: expert: 16 (over y, z), width: 8 (over x, core).
Axes of the slice: x: 4, y: 4, z: 4, core: 2. Of those that a mesh axis runs over, the one named last changes fastest.
Arguments:
- tokens_in: bfloat16 [6144, 7168], P('expert', 'width'), may hold values from -6 to 6
- out_grad: bfloat16 [6144, 7168], P('expert', 'width'), may hold values from -0.08984375 to 0.08984375
- router_weight: bfloat16 [7168, 256], P('width'), may hold values from -0.0625 to 0.0625
- expert_out: bfloat16 [49152, 7168], P('expert', 'width'), may hold values from -6 to 6
- expert_ids: int32 [6144, 8], P('expert'), may hold values from 0 to 255, as said below
- slot_ids: int32 [6144, 8], P('expert'), may hold values from 0 to 191, as said below
Outputs:
- expert_grad: bfloat16 [49152, 7168], P('expert', 'width')
- router_grad: float32 [7168, 256], P('width', 'expert')
- input_grad: bfloat16 [6144, 7168], P('expert', 'width')
The draws below stay inside these ranges and needn't reach their ends.
Inputs may be any that keep to these rules, and one draw needn't show every extreme that they name: `expert_ids`: expert e lies on device e // 16 of the expert axis; a token's 8 experts lie on 8 different devices. The tokens of each device choose experts of each device of the expert axis exactly 192 times. slot_ids[t, k] is the row, within the block of 192 rows that token t's device sends to the device of expert expert_ids[t, k], of that pair. The pairs of one block fill all its rows, grouped by expert in rising order and by token in rising order within an expert. The values of expert_ids and slot_ids fit in 8 bits each, and both may be sent packed several to a 32-bit word.
All inputs are finite; a program needn't handle non-finite values.
Results may differ from the reference program's by a relative error of at most 0.015.
Values may be sent and summed in bfloat16 or wider, within the bound.
No kernel may reach another device: no remote copies, remote signals or barrier semaphores. Data moves between devices by JAX's collectives and lax.ppermute only.
A program may use at most 128 MiB of HBM per device.

```python
import jax
import jax.numpy as jnp

D = 7168
EXP_DEV = 16
TOPK = 8
TOK_DEV = 384
TOKENS = 6144
EXPERTS = 256
CAP = 192
RECV = 49152
N_EXPERT = 16


def make_routes(key):
    base = jax.random.fold_in(key, 7)
    key_dev, key_tok, key_local = jax.random.split(base, 3)
    groups = TOKENS // TOK_DEV
    device_count = EXPERTS // EXP_DEV
    dev_rank = jax.random.randint(key_dev, (groups, device_count), 0, 1048576, dtype=jnp.int32) * device_count + jnp.arange(device_count, dtype=jnp.int32)[None, :]
    dev_perm = jnp.argsort(dev_rank, axis=1).astype(jnp.int32)
    tok_rank = jax.random.randint(key_tok, (groups, TOK_DEV), 0, 1048576, dtype=jnp.int32) * TOK_DEV + jnp.arange(TOK_DEV, dtype=jnp.int32)[None, :]
    tok_perm = jnp.argsort(tok_rank, axis=1).astype(jnp.int32)
    offsets = (tok_perm[:, :, None] + jnp.arange(TOPK, dtype=jnp.int32)[None, None, :]) % device_count
    chosen = jnp.take_along_axis(dev_perm, offsets.reshape(groups, TOK_DEV * TOPK), axis=1).reshape(TOKENS, TOPK)
    local_ids = jax.random.randint(key_local, (TOKENS, TOPK), 0, EXP_DEV, dtype=jnp.int32)
    expert_ids = chosen * EXP_DEV + local_ids
    matches = expert_ids[:, :, None] == jnp.arange(EXPERTS, dtype=jnp.int32)[None, None, :]
    routed = jnp.sum(matches.astype(jnp.int32), axis=1).reshape(groups, TOK_DEV, EXPERTS)
    before = jnp.cumsum(routed, axis=1) - routed
    counts = jnp.sum(routed, axis=1).reshape(groups, device_count, EXP_DEV)
    offset = (jnp.cumsum(counts, axis=2) - counts).reshape(groups, 1, EXPERTS)
    positions = (offset + before).reshape(TOKENS, EXPERTS)
    slot_ids = jnp.take_along_axis(positions, expert_ids, axis=1).astype(jnp.int32)
    return (expert_ids.astype(jnp.int32), slot_ids)


def draw_expert_ids(key, part):
    return make_routes(key)[0]


def draw_slot_ids(key, part):
    return make_routes(key)[1]


def block_scale(stream_key, shape, cuts, smallest, top_value):
    loudness, own = 1.0, jax.random.fold_in(stream_key, 6)
    for axis_at, shards_of in cuts:
        draws = jnp.exp(jax.random.uniform(jax.random.fold_in(own, axis_at), (shards_of,), jnp.float32, smallest / len(cuts), top_value / len(cuts)))
        loudness = loudness * jnp.repeat(draws, shape[axis_at] // shards_of).reshape([-1 if axis == axis_at else 1 for axis in range(len(shape))])
    return loudness


def centred(rng, extent, deviation, most, cuts=(), kind=jnp.bfloat16):
    values = deviation * jax.random.normal(rng, extent, jnp.float32)
    if cuts:
        values = values * block_scale(rng, extent, cuts, -0.22, 0.18)
    return jnp.clip(values, -most, most).astype(kind)


def setup_inputs(seed: int = 0) -> dict:
    key_of = jax.random.split(jax.random.key(seed), 7)
    tokens_in = centred(key_of[0], (TOKENS, D), 1.0, 6.0, ((0, 16), (1, 8)))
    out_grad = centred(key_of[1], (TOKENS, D), 0.015, 0.08984375, ((0, 16), (1, 8)))
    router_weight = centred(key_of[2], (D, EXPERTS), D ** -0.5, 0.0625, ((0, 8),))
    expert_out = centred(key_of[3], (RECV, D), 1.0, 6.0, ((0, 16), (1, 8)))
    expert_ids = draw_expert_ids(jax.random.fold_in(key_of[6], 71), 0)
    slot_ids = draw_slot_ids(jax.random.fold_in(key_of[6], 71), 0)
    return {"tokens_in": tokens_in, "out_grad": out_grad, "router_weight": router_weight, "expert_out": expert_out, "expert_ids": expert_ids, "slot_ids": slot_ids}


route_scale = 2.5


def gate_parts(logits, expert_ids):
    scores = jax.nn.sigmoid(logits)
    picked = jnp.take_along_axis(scores, expert_ids, axis=1)
    totals = jnp.sum(picked, axis=1, keepdims=True)
    return picked, totals


def logit_gradient(gate_grads, picked, totals, expert_ids, expert_count):
    weighted = jnp.sum(gate_grads * picked, axis=1, keepdims=True) / totals
    score_grads = route_scale / totals * (gate_grads - weighted)
    local_grads = score_grads * picked * (1.0 - picked)
    matches = expert_ids[:, :, None] == jnp.arange(expert_count, dtype=jnp.int32)[None, None, :]
    return jnp.sum(jnp.where(matches, local_grads[:, :, None], 0.0), axis=1).astype(jnp.bfloat16)


def reference(tokens_in, out_grad, router_weight, expert_out, expert_ids, slot_ids):
    logits = jnp.dot(tokens_in, router_weight, preferred_element_type=jnp.float32)
    picked, totals = gate_parts(logits, expert_ids)
    gate_weights = (route_scale * picked / totals).astype(jnp.bfloat16)
    source = (jnp.arange(TOKENS, dtype=jnp.int32) // TOK_DEV).astype(jnp.int32)
    row_of = ((expert_ids // EXP_DEV) * (N_EXPERT * CAP) + source[:, None] * CAP + slot_ids).astype(jnp.int32)
    grad_f32 = out_grad.astype(jnp.float32)
    expert_grad = jnp.zeros((RECV, D), jnp.bfloat16)
    columns = []
    for pick in range(TOPK):
        outputs = expert_out[row_of[:, pick]].astype(jnp.float32)
        columns.append(jnp.sum(outputs * grad_f32, axis=1))
        update = (gate_weights[:, pick].astype(jnp.float32)[:, None] * grad_f32).astype(jnp.bfloat16)
        expert_grad = expert_grad.at[row_of[:, pick]].set(update)
    gate_grads = jnp.stack(columns, axis=1)
    logit_grads = logit_gradient(gate_grads, picked, totals, expert_ids, EXPERTS)
    router_grad = jnp.dot(tokens_in.T, logit_grads, preferred_element_type=jnp.float32)
    input_grad = jnp.dot(logit_grads, router_weight.T, preferred_element_type=jnp.float32).astype(jnp.bfloat16)
    return (expert_grad, router_grad, input_grad)
```

```python
import functools

import jax
import jax.numpy as jnp
from jax import lax
from jax.experimental import pallas as pl
from jax.experimental.pallas import tpu as pltpu
from jax.sharding import PartitionSpec as P

route_scale = 2.5
AXES = ("expert", "width")
f32, bf16, i32 = jnp.float32, jnp.bfloat16, jnp.int32


def grid_sides(n_expert):
    side = int(round(n_expert**0.5))
    return side


def line_shift(n_expert, n_width, shift, second):
    side = grid_sides(n_expert)
    pairs = []
    for e in range(n_expert):
        y, z = e // side, e % side
        for w in range(n_width):
            if (w % 2 == 0) != second:
                to = ((y + shift) % side) * side + z
            else:
                to = y * side + (z + shift) % side
            pairs.append((e * n_width + w, to * n_width + w))
    return pairs


def picked_kernel(ids_ref, tok_ref, w_ref, out_ref):
    logits = lax.dot_general(
        w_ref[...], tok_ref[...], (((0,), (1,)), ((), ())), preferred_element_type=f32
    )
    experts = lax.broadcasted_iota(i32, logits.shape, 0)
    rows = []
    for k in range(ids_ref.shape[0]):
        hit = experts == ids_ref[k : k + 1, :]
        rows.append(jnp.sum(jnp.where(hit, logits, 0.0), axis=0, keepdims=True))
    out_ref[...] = jnp.concatenate(rows, axis=0)


def gates_of(parts):
    logits = jnp.sum(parts, axis=0)
    picked = 1.0 / (1.0 + jnp.exp(-logits))
    totals = jnp.sum(picked, axis=0, keepdims=True)
    exact = route_scale * picked / totals
    return picked, totals, exact


def gate_kernel(per_device, parts_ref, ids_ref, slots_ref, out_ref):
    _, _, exact = gates_of(parts_ref[...])
    dev = ids_ref[...] // per_device
    out_ref[...] = jnp.concatenate(
        [dev.astype(f32), slots_ref[...].astype(f32), exact.astype(bf16).astype(f32)], axis=0
    )


def compact_kernel(n_src, top, cap, dest_ref, *refs):
    info_refs, x_refs, out_refs = refs[:n_src], refs[n_src : 2 * n_src], refs[2 * n_src :]
    for d in range(len(out_refs)):
        dest = dest_ref[d].astype(f32)
        for j in range(n_src):
            info = info_refs[j][...]
            here = info[:top] == dest
            slot = jnp.sum(jnp.where(here, info[top : 2 * top] + 1.0, 0.0), axis=0, keepdims=True)
            gate = jnp.sum(jnp.where(here, info[2 * top :], 0.0), axis=0, keepdims=True)
            rows = lax.broadcasted_iota(i32, (cap, slot.shape[1]), 0)
            table = jnp.where(rows == slot.astype(i32) - 1, gate, 0.0).astype(bf16)
            got = jnp.dot(table, x_refs[j][...], preferred_element_type=f32)
            out_refs[d][j * cap : (j + 1) * cap, :] = got.astype(bf16)


def compact(dests, infos, xs, top, cap, n_dest):
    n_src = len(xs)
    tok, width = xs[0].shape
    whole = pl.BlockSpec(memory_space=pltpu.VMEM)
    return pl.pallas_call(
        functools.partial(compact_kernel, n_src, top, cap),
        out_shape=[jax.ShapeDtypeStruct((n_src * cap, width), bf16)] * n_dest,
        in_specs=[pl.BlockSpec(memory_space=pltpu.SMEM)] + [whole] * (2 * n_src),
        out_specs=[whole] * n_dest,
        cost_estimate=pl.CostEstimate(
            flops=2 * n_src * n_dest * cap * tok * width, bytes_accessed=n_src * tok * width * 6, transcendentals=0
        ),
        name="compact",
    )(dests, *infos, *xs)


def land_kernel(src_ref, chunk_ref, eo_ref, *refs):
    out_ref, dot_ref = refs[-2:]
    chunk = chunk_ref[...]
    out_ref[...] = chunk
    width = chunk.shape[1]
    total = None
    for at in range(0, width, 128):
        term = chunk[:, at : at + 128].astype(f32) * eo_ref[:, at : at + 128].astype(f32)
        total = term if total is None else total + term
    dots = jnp.sum(total.T, axis=0, keepdims=True)
    dot_ref[...] = jnp.broadcast_to(dots[None], dot_ref.shape)


def land(srcs, chunk, expert_out, grad, dots, cap, n_width):
    rows, width = chunk.shape
    n = rows // cap
    buffer_rows = expert_out.shape[0]
    held = [] if grad is None else [grad, dots]
    return pl.pallas_call(
        land_kernel,
        grid_spec=pltpu.PrefetchScalarGridSpec(
            num_scalar_prefetch=1,
            grid=(n,),
            in_specs=[
                pl.BlockSpec((cap, width), lambda i, s: (i, 0)),
                pl.BlockSpec((cap, width), lambda i, s: (s[i], 0)),
            ]
            + [pl.BlockSpec(memory_space=pl.ANY)] * len(held),
            out_specs=[
                pl.BlockSpec((cap, width), lambda i, s: (s[i], 0)),
                pl.BlockSpec((n_width, 1, cap), lambda i, s: (s[i], 0, 0)),
            ],
        ),
        out_shape=[
            jax.ShapeDtypeStruct((buffer_rows, width), bf16),
            jax.ShapeDtypeStruct((buffer_rows // cap * n_width, 1, cap), f32),
        ],
        input_output_aliases={3: 0, 4: 1} if held else {},
        cost_estimate=pl.CostEstimate(flops=2 * rows * width, bytes_accessed=6 * rows * width, transcendentals=0),
        name="land",
    )(srcs, chunk, expert_out, *held)


def tail_kernel(n_expert, n_width, per_device, got_ref, parts_ref, ids_ref, slots_ref, tok_ref, lg_ref, router_ref):
    top, tok = ids_ref.shape
    cap = got_ref.shape[2]
    rows = []
    for e in range(n_expert):
        row = got_ref[e * n_width]
        for w in range(1, n_width):
            row = row + got_ref[e * n_width + w]
        rows.append(row)
    dots = jnp.concatenate(rows, axis=0)
    high = dots.astype(bf16)
    rest = dots - high.astype(f32)
    middle = rest.astype(bf16)
    both = jnp.concatenate([high, middle], axis=0)
    ids, slots = ids_ref[...], slots_ref[...]
    dev = ids // per_device
    slot_rows = lax.broadcasted_iota(i32, (cap, tok), 0)
    dev_rows = lax.broadcasted_iota(i32, (n_expert, tok), 0)
    out = []
    for k in range(top):
        table = jnp.where(slot_rows == slots[k : k + 1], 1.0, 0.0).astype(bf16)
        found = jnp.dot(both, table, preferred_element_type=f32)
        found = found[:n_expert] + found[n_expert:]
        out.append(jnp.sum(jnp.where(dev_rows == dev[k : k + 1], found, 0.0), axis=0, keepdims=True))
    scaled = jnp.concatenate(out, axis=0)
    picked, totals, exact = gates_of(parts_ref[...])
    sent = exact.astype(bf16).astype(f32)
    scaled = scaled * jnp.where(sent > 0.0, exact / jnp.where(sent > 0.0, sent, 1.0), 1.0)
    mean = jnp.sum(scaled, axis=0, keepdims=True) / totals
    local = (1.0 - picked) * (scaled - picked * mean)
    experts = lax.broadcasted_iota(i32, (lg_ref.shape[0], tok), 0)
    grads = jnp.zeros(lg_ref.shape, f32)
    for k in range(top):
        grads = grads + jnp.where(experts == ids[k : k + 1], local[k : k + 1], 0.0)
    grads = grads.astype(bf16)
    lg_ref[...] = grads
    router_ref[...] = jnp.dot(grads, tok_ref[...], preferred_element_type=f32).astype(bf16)


def body(tokens_in, out_grad, router_weight, expert_out, expert_ids, slot_ids):
    n_expert, n_width = lax.axis_size("expert"), lax.axis_size("width")
    side = grid_sides(n_expert)
    tok, width = out_grad.shape
    top = expert_ids.shape[1]
    experts = router_weight.shape[1]
    per_device = experts // n_expert
    cap = tok * top // n_expert
    me, core = lax.axis_index("expert"), lax.axis_index("width") % 2
    y, z = me // side, me % side

    def cell(along, across):
        first = ((y + along) % side) * side + (z + across) % side
        second = ((y + across) % side) * side + (z + along) % side
        return jnp.where(core == 0, first, second).astype(i32)

    def send(x, shift, second):
        return lax.ppermute(x, AXES, line_shift(n_expert, n_width, shift, second))

    shifts = list(range(1, side))
    xs = {0: out_grad}
    for s in (1, side - 1) + tuple(range(2, side - 1)):
        xs[s] = send(out_grad, s, False)

    ids, slots = expert_ids.T, slot_ids.T
    vmem = pl.BlockSpec(memory_space=pltpu.VMEM)
    part = pl.pallas_call(
        picked_kernel,
        out_shape=jax.ShapeDtypeStruct((top, tok), f32),
        in_specs=[vmem] * 3,
        out_specs=vmem,
        cost_estimate=pl.CostEstimate(flops=2 * tok * width * experts, bytes_accessed=2 * tok * width, transcendentals=0),
        name="picked",
    )(ids, tokens_in, router_weight)
    parts = lax.all_to_all(jnp.broadcast_to(part[None], (n_width, top, tok)), "width", 0, 0, tiled=True)
    info = pl.pallas_call(
        functools.partial(gate_kernel, per_device),
        out_shape=jax.ShapeDtypeStruct((3 * top, tok), f32),
        in_specs=[vmem] * 3,
        out_specs=vmem,
        name="gates",
    )(parts, ids, slots)
    infos = {0: info}
    for s in shifts:
        infos[s] = send(info, s, False)

    dests = jnp.stack([cell(0, d) for d in range(side)])
    batches = [[0], [1, side - 1]] + [[s] for s in range(2, side - 1)]
    grad, dots = None, None
    landed = []
    for batch in batches:
        chunks = compact(dests, [infos[s] for s in batch], [xs[s] for s in batch], top, cap, side)
        for d in range(side):
            moved = chunks[d] if d == 0 else send(chunks[d], d, True)
            srcs = jnp.stack([cell(-s, -d) for s in batch])
            landed.append((srcs, moved))
    for srcs, moved in landed:
        grad, dots = land(srcs, moved, expert_out, grad, dots, cap, n_width)

    got = lax.all_to_all(dots, AXES, 0, 0, tiled=True)
    logit_grads, router_part = pl.pallas_call(
        functools.partial(tail_kernel, n_expert, n_width, per_device),
        out_shape=[
            jax.ShapeDtypeStruct((experts, tok), bf16),
            jax.ShapeDtypeStruct((experts, width), bf16),
        ],
        in_specs=[vmem] * 5,
        out_specs=[vmem] * 2,
        cost_estimate=pl.CostEstimate(flops=2 * tok * width * experts, bytes_accessed=2 * tok * width, transcendentals=0),
        name="tail",
    )(got, parts, ids, slots, tokens_in)
    blocks = lax.all_to_all(router_part.reshape(n_expert, per_device, width), "expert", 0, 0, tiled=True)
    input_grad = lax.dot_general(
        logit_grads, router_weight, (((0,), (1,)), ((), ())), preferred_element_type=f32
    ).astype(bf16)
    router_grad = jnp.sum(blocks.astype(f32), axis=0).T
    return (grad, router_grad, input_grad)


def solution(mesh):
    return jax.shard_map(
        body,
        mesh=mesh,
        in_specs=(
            P("expert", "width"),
            P("expert", "width"),
            P("width", None),
            P("expert", "width"),
            P("expert", None),
            P("expert", None),
        ),
        out_specs=(P("expert", "width"), P("width", "expert"), P("expert", "width")),
        check_vma=False,
    )
```

```python
import functools

import jax
import jax.numpy as jnp
from jax import lax
from jax.experimental import pallas as pl
from jax.experimental.pallas import tpu as pltpu
from jax.sharding import PartitionSpec as P


route_scale = 2.5
AXES = ("expert", "width")
f32, bf16, i32 = jnp.float32, jnp.bfloat16, jnp.int32
VMEM = pl.BlockSpec(memory_space=pltpu.VMEM)
SMEM = pl.BlockSpec(memory_space=pltpu.SMEM)
ANY = pl.BlockSpec(memory_space=pl.ANY)
HBM = pl.BlockSpec(memory_space=pltpu.HBM)


def params(mib):
    return pltpu.CompilerParams(vmem_limit_bytes=mib * 1024 * 1024)


def cost(flops, moved):
    return pl.CostEstimate(flops=flops, bytes_accessed=moved, transcendentals=0)


def line_shift(n_expert, n_width, shift, second):
    side = int(round(n_expert**0.5))
    pairs = []
    for e in range(n_expert):
        y, z = e // side, e % side
        for w in range(n_width):
            if (w % 2 == 0) != second:
                to = ((y + shift) % side) * side + z
            else:
                to = y * side + (z + shift) % side
            pairs.append((e * n_width + w, to * n_width + w))
    return pairs


def here():
    n_expert = lax.axis_size("expert")
    side = int(round(n_expert**0.5))
    me = lax.axis_index("expert")
    return side, lax.div(me, side), lax.rem(me, side), lax.rem(lax.axis_index("width"), 2)


def cell(place, along, across):
    side, y, z, core = place
    along, across = along % side, across % side
    first = lax.rem(y + along, side) * side + lax.rem(z + across, side)
    second = lax.rem(y + across, side) * side + lax.rem(z + along, side)
    return jnp.where(core == 0, first, second)


def in_hbm(x):
    return pltpu.with_memory_space_constraint(x, pltpu.HBM)


def pack_kernel(per_device, x_ref, ids_ref, slots_ref, out_ref):
    tok, width = x_ref.shape
    top = ids_ref.shape[0]
    out_ref[:tok, :] = x_ref[...]
    dev = (ids_ref[...] // per_device).astype(f32)
    slots = slots_ref[...].astype(f32)
    rest = jnp.zeros((top, width - 2 * tok), f32)
    out_ref[tok:, :] = jnp.concatenate([dev, slots, rest], axis=1).astype(bf16)


def compact_kernel(n_src, tok, cap, n_dest, *refs):
    x_refs, (stage, sem), out_refs = refs[:n_src], refs[-2:], refs[-2 - n_dest : -2]
    place = here()
    copies = []
    for d in list(range(1, n_dest)) + [0]:
        for j in range(n_src):
            info = x_refs[j][tok:, :].astype(f32)
            dev, slots = info[:, :tok], info[:, tok : 2 * tok]
            mine = dev == cell(place, 0, d).astype(f32)
            slot = jnp.sum(jnp.where(mine, slots + 1.0, 0.0), axis=0, keepdims=True)
            rows = lax.broadcasted_iota(i32, (cap, tok), 0)
            table = jnp.where(rows == slot.astype(i32) - 1, 1.0, 0.0).astype(bf16)
            got = jnp.dot(table, x_refs[j][:tok, :], preferred_element_type=f32)
            stage[d, j * cap : (j + 1) * cap, :] = got.astype(bf16)
        copies.append(pltpu.make_async_copy(stage.at[d], out_refs[d], sem.at[d]))
        copies[-1].start()
    for copy in copies:
        copy.wait()


def compact(xs, after, tok, cap, n_dest):
    n_src, width = len(xs), xs[0].shape[1]
    return pl.pallas_call(
        functools.partial(compact_kernel, n_src, tok, cap, n_dest),
        out_shape=[pltpu.HBM((n_src * cap, width), bf16)] * n_dest,
        in_specs=[VMEM] * n_src + [ANY] * len(after),
        out_specs=[HBM] * n_dest,
        scratch_shapes=[
            pltpu.VMEM((n_dest, n_src * cap, width), bf16),
            pltpu.SemaphoreType.DMA((n_dest,)),
        ],
        compiler_params=params(8),
        cost_estimate=cost(2 * n_src * n_dest * cap * tok * width, n_src * tok * width * 6),
        name="compact",
    )(*xs, *map(in_hbm, after))


def picked_kernel(ids_ref, tok_ref, w_ref, after_ref, out_ref):
    logits = lax.dot_general(
        w_ref[...], tok_ref[...], (((0,), (1,)), ((), ())), preferred_element_type=f32
    )
    experts = lax.broadcasted_iota(i32, logits.shape, 0)
    rows = []
    for k in range(ids_ref.shape[0]):
        hit = experts == ids_ref[k : k + 1, :]
        rows.append(jnp.sum(jnp.where(hit, logits, 0.0), axis=0, keepdims=True))
    picked = jnp.concatenate(rows, axis=0)
    for w in range(out_ref.shape[0]):
        out_ref[w] = picked


def front(ids, tokens_in, router_weight, after, n_width):
    (top, tok), width, experts = ids.shape, tokens_in.shape[1], router_weight.shape[1]
    return pl.pallas_call(
        picked_kernel,
        out_shape=jax.ShapeDtypeStruct((n_width, top, tok), f32),
        in_specs=[VMEM] * 3 + [HBM],
        out_specs=VMEM,
        compiler_params=params(4),
        cost_estimate=cost(2 * tok * width * experts, 2 * tok * width),
        name="picked",
    )(ids, tokens_in, router_weight, in_hbm(after))


def gates_of(parts):
    logits = jnp.sum(parts, axis=0)
    picked = 1.0 / (1.0 + jnp.exp(-logits))
    totals = jnp.sum(picked, axis=0, keepdims=True)
    return picked, totals


def gate_kernel(per_device, parts_ref, ids_ref, slots_ref, out_ref):
    picked, totals = gates_of(parts_ref[...])
    gates = (route_scale * picked / totals).astype(bf16).astype(f32)
    top, tok = ids_ref.shape
    n_expert, cap = out_ref.shape
    dev, slots = ids_ref[...] // per_device, slots_ref[...]
    dev_rows = lax.broadcasted_iota(i32, (n_expert, tok), 0)
    slot_rows = lax.broadcasted_iota(i32, (cap, tok), 0)
    total = jnp.zeros((n_expert, cap), f32)
    for k in range(top):
        left = jnp.where(dev_rows == dev[k : k + 1], gates[k : k + 1], 0.0).astype(bf16)
        right = jnp.where(slot_rows == slots[k : k + 1], 1.0, 0.0).astype(bf16)
        total = total + lax.dot_general(left, right, (((1,), (1,)), ((), ())), preferred_element_type=f32)
    out_ref[...] = total


def row_dots(chunk, other):
    total = None
    for at in range(0, chunk.shape[1], 128):
        term = chunk[:, at : at + 128].astype(f32) * other[:, at : at + 128].astype(f32)
        total = term if total is None else total + term
    return jnp.sum(total.T, axis=0, keepdims=True)


def fetch(eo_ref, stage, sem, cells, cap):
    copies = []
    for at, src in enumerate(cells):
        rows = eo_ref.at[pl.ds(pl.multiple_of(src * cap, cap), cap), :]
        copies.append(pltpu.make_async_copy(rows, stage.at[at], sem.at[at]))
        copies[-1].start()
    return copies


def fetch_chunks(chunk_refs, stage, sem, cap, first=0):
    copies, at = [], first
    for chunk_ref in chunk_refs:
        for j in range(chunk_ref.shape[0] // cap):
            copies.append(pltpu.make_async_copy(chunk_ref.at[pl.ds(j * cap, cap), :], stage.at[at], sem.at[at]))
            copies[-1].start()
            at += 1
    return copies


def cells_of(batch, side, place):
    return [cell(place, -s, -d) for d in range(side) for s in batch]


def dots_kernel(batch, side, cap, next_batch, eo_ref, *refs):
    chunk_refs = refs[:side]
    out_refs, (held, stage, sem, next_sem) = refs[side:-4], refs[-4:]
    place = here()
    rows = fetch_chunks(chunk_refs, held, sem.at[0], cap)
    others = fetch(eo_ref, stage, sem.at[1], cells_of(batch, side, place), cap)
    ahead = fetch(eo_ref, out_refs[1], next_sem, cells_of(next_batch, side, place), cap) if next_batch else []
    for at in range(len(rows)):
        rows[at].wait()
        others[at].wait()
        out_refs[0][at : at + 1, :] = row_dots(held.at[at], stage.at[at])
    for copy in ahead:
        copy.wait()


def row_dots_call(batch, next_batch, eo, chunks, cap):
    n, width, side = len(batch) * len(chunks), chunks[0].shape[1], len(chunks)
    n_next = len(next_batch) * side
    outs = [jax.ShapeDtypeStruct((n, cap), f32)]
    if n_next:
        outs.append(pltpu.VMEM((n_next, cap, width), bf16))
    return pl.pallas_call(
        functools.partial(dots_kernel, batch, side, cap, next_batch),
        out_shape=outs,
        in_specs=[HBM] * (1 + side),
        out_specs=[VMEM] * len(outs),
        scratch_shapes=[
            pltpu.VMEM((n, cap, width), bf16),
            pltpu.VMEM((n, cap, width), bf16),
            pltpu.SemaphoreType.DMA((2, n)),
            pltpu.SemaphoreType.DMA((max(n_next, 1),)),
        ],
        compiler_params=params(8),
        cost_estimate=cost(2 * n * cap * width, 4 * n * cap * width),
        name="dots",
    )(in_hbm(eo), *map(in_hbm, chunks))


def last_dots_kernel(n_width, batches, cap, side, gate_ref, eo_ref, *refs):
    chunk_refs, early_refs, (out_ref, held, sem) = refs[:side], refs[side:-3], refs[-3:]
    n_expert = gate_ref.shape[0]
    place = here()
    copies = fetch_chunks(chunk_refs, held, sem, cap)
    for e in range(n_expert):
        for w in range(n_width):
            out_ref[2 * (e * n_width + w) + 1] = gate_ref[e : e + 1, :]

    def put(src, row):
        base = src * (2 * n_width)
        for w in range(n_width):
            out_ref[base + 2 * w] = row

    for batch, early in zip(batches[:-1], early_refs):
        for at, src in enumerate(cells_of(batch, side, place)):
            put(src, early[at : at + 1, :])
    for at, src in enumerate(cells_of(batches[-1], side, place)):
        copies[at].wait()
        put(src, row_dots(held.at[at], eo_ref.at[at]))


def tail_kernel(n_expert, n_width, per_device, got_ref, parts_ref, ids_ref, slots_ref, tok_ref, lg_ref, router_ref):
    top, tok = ids_ref.shape
    rows = []
    for e in range(n_expert):
        row = got_ref[2 * e * n_width]
        for w in range(1, n_width):
            row = row + got_ref[2 * (e * n_width + w)]
        rows.append(row)
    dots = jnp.concatenate(rows, axis=0)
    cap = dots.shape[1]
    high = dots.astype(bf16)
    low = (dots - high.astype(f32)).astype(bf16)
    both = jnp.concatenate([high, low], axis=0)
    ids, slots = ids_ref[...], slots_ref[...]
    dev = ids // per_device
    slot_rows = lax.broadcasted_iota(i32, (cap, tok), 0)
    dev_rows = lax.broadcasted_iota(i32, (n_expert, tok), 0)
    out = []
    for k in range(top):
        table = jnp.where(slot_rows == slots[k : k + 1], 1.0, 0.0).astype(bf16)
        found = jnp.dot(both, table, preferred_element_type=f32)
        found = found[:n_expert] + found[n_expert:]
        out.append(jnp.sum(jnp.where(dev_rows == dev[k : k + 1], found, 0.0), axis=0, keepdims=True))
    gate_grads = jnp.concatenate(out, axis=0)
    picked, totals = gates_of(parts_ref[...])
    weighted = jnp.sum(gate_grads * picked, axis=0, keepdims=True) / totals
    local = route_scale / totals * (gate_grads - weighted) * picked * (1.0 - picked)
    experts = lax.broadcasted_iota(i32, (lg_ref.shape[0], tok), 0)
    grads = jnp.zeros(lg_ref.shape, f32)
    for k in range(top):
        grads = grads + jnp.where(experts == ids[k : k + 1], local[k : k + 1], 0.0)
    grads = grads.astype(bf16)
    lg_ref[...] = grads
    router_ref[...] = jnp.dot(grads, tok_ref[...], preferred_element_type=f32).astype(bf16)


def scale_kernel(n_width, batches, cap, side, got_ref, lg_ref, w_ref, *refs):
    chunk_refs, (out_ref, input_ref, held, stage, in_sem, sem) = refs[:-6], refs[-6:]
    place = here()
    rows = fetch_chunks(chunk_refs, held, in_sem, cap)
    copies = []
    cells = sum([cells_of(batch, side, place) for batch in batches], [])
    for at, src in enumerate(cells):
        gate = jnp.broadcast_to(got_ref[src * (2 * n_width) + 1], (128, cap)).T
        rows[at].wait()
        for lane in range(0, held.shape[2], 128):
            part = held[at, :, lane : lane + 128].astype(f32)
            stage[at, :, lane : lane + 128] = (part * gate).astype(bf16)
        to = out_ref.at[pl.ds(pl.multiple_of(src * cap, cap), cap), :]
        copies.append(pltpu.make_async_copy(stage.at[at], to, sem.at[at]))
        copies[-1].start()
    input_ref[...] = lax.dot_general(
        lg_ref[...], w_ref[...], (((0,), (1,)), ((), ())), preferred_element_type=f32
    ).astype(bf16)
    for copy in copies:
        copy.wait()


def body(tokens_in, out_grad, router_weight, expert_out, expert_ids, slot_ids):
    n_expert, n_width = lax.axis_size("expert"), lax.axis_size("width")
    side = int(round(n_expert**0.5))
    tok, width = out_grad.shape
    top = expert_ids.shape[1]
    experts = router_weight.shape[1]
    per_device = experts // n_expert
    cap = tok * top // n_expert

    def send(x, shift, second):
        return lax.ppermute(x, AXES, line_shift(n_expert, n_width, shift, second))

    ids, slots = expert_ids.T, slot_ids.T
    packed = pl.pallas_call(
        functools.partial(pack_kernel, per_device),
        out_shape=jax.ShapeDtypeStruct((tok + top, width), bf16),
        in_specs=[VMEM] * 3,
        out_specs=VMEM,
        compiler_params=params(4),
        cost_estimate=cost(0, 4 * tok * width),
        name="pack",
    )(out_grad, ids, slots)
    batches = [[0], [1, side - 1]] + [[s] for s in range(2, side - 1)]
    xs = {0: packed}
    for batch in batches[1:]:
        for s in batch:
            xs[s] = send(packed, s, False)

    landed, after = [], []
    for batch in batches:
        chunks = compact([xs[s] for s in batch], after, tok, cap, side)
        after = [chunks[0]]
        group = [chunks[0]]
        for d in range(1, side):
            group.append(send(chunks[d], d, True))
        landed.append(group)

    sent_parts = front(ids, tokens_in, router_weight, after[0], n_width)
    parts = lax.all_to_all(sent_parts, "width", 0, 0, tiled=True)
    gates = pl.pallas_call(
        functools.partial(gate_kernel, per_device),
        out_shape=jax.ShapeDtypeStruct((n_expert, cap), f32),
        in_specs=[VMEM] * 3,
        out_specs=VMEM,
        compiler_params=params(4),
        cost_estimate=cost(2 * top * n_expert * cap * tok, 4 * n_width * top * tok),
        name="gates",
    )(parts, ids, slots)

    early = []
    for b, batch in enumerate(batches[:-1]):
        next_batch = batches[-1] if b == len(batches) - 2 else []
        outs = row_dots_call(batch, next_batch, expert_out, landed[b], cap)
        early.append(outs[0])
    sent = pl.pallas_call(
        functools.partial(last_dots_kernel, n_width, batches, cap, side),
        out_shape=jax.ShapeDtypeStruct((2 * n_expert * n_width, 1, cap), f32),
        in_specs=[VMEM] * 2 + [HBM] * side + [VMEM] * len(early),
        out_specs=VMEM,
        scratch_shapes=[
            pltpu.VMEM((side, cap, width), bf16),
            pltpu.SemaphoreType.DMA((side,)),
        ],
        compiler_params=params(6),
        cost_estimate=cost(2 * side * cap * width, 4 * side * cap * width),
        name="last_dots",
    )(gates, outs[1], *map(in_hbm, landed[-1]), *early)
    got = lax.all_to_all(sent, AXES, 0, 0, tiled=True)

    logit_grads, router_part = pl.pallas_call(
        functools.partial(tail_kernel, n_expert, n_width, per_device),
        out_shape=[
            jax.ShapeDtypeStruct((experts, tok), bf16),
            jax.ShapeDtypeStruct((experts, width), bf16),
        ],
        in_specs=[VMEM] * 5,
        out_specs=[VMEM] * 2,
        compiler_params=params(8),
        cost_estimate=cost(2 * tok * width * experts, 2 * tok * width),
        name="tail",
    )(got, parts, ids, slots, tokens_in)
    blocks = lax.all_to_all(router_part.reshape(n_expert, per_device, width), "expert", 0, 0, tiled=True)
    flat = sum(landed, [])
    expert_grad, input_grad = pl.pallas_call(
        functools.partial(scale_kernel, n_width, batches, cap, side),
        out_shape=[
            jax.ShapeDtypeStruct(expert_out.shape, bf16),
            jax.ShapeDtypeStruct((tok, width), bf16),
        ],
        in_specs=[VMEM] * 3 + [HBM] * len(flat),
        out_specs=[HBM, VMEM],
        scratch_shapes=[
            pltpu.VMEM((n_expert, cap, width), bf16),
            pltpu.VMEM((n_expert, cap, width), bf16),
            pltpu.SemaphoreType.DMA((n_expert,)),
            pltpu.SemaphoreType.DMA((n_expert,)),
        ],
        compiler_params=params(16),
        cost_estimate=cost(2 * tok * width * experts, 4 * n_expert * cap * width),
        name="scale",
    )(got, logit_grads, router_weight, *map(in_hbm, flat))
    router_grad = jnp.sum(blocks.astype(f32), axis=0).T
    return (expert_grad, router_grad, input_grad)


def solution(mesh):
    return jax.shard_map(
        body,
        mesh=mesh,
        in_specs=(
            P("expert", "width"),
            P("expert", "width"),
            P("width", None),
            P("expert", "width"),
            P("expert", None),
            P("expert", None),
        ),
        out_specs=(P("expert", "width"), P("width", "expert"), P("expert", "width")),
        check_vma=False,
    )
```

```python
import functools

import jax
import jax.numpy as jnp
from jax import lax
from jax.experimental import pallas as pl
from jax.experimental.pallas import tpu as pltpu
from jax.sharding import PartitionSpec as P


route_scale = 2.5
AXES = ("expert", "width")
f32, bf16, i32 = jnp.float32, jnp.bfloat16, jnp.int32
VMEM = pl.BlockSpec(memory_space=pltpu.VMEM)
SMEM = pl.BlockSpec(memory_space=pltpu.SMEM)
ANY = pl.BlockSpec(memory_space=pl.ANY)
HBM = pl.BlockSpec(memory_space=pltpu.HBM)


def params(mib):
    return pltpu.CompilerParams(vmem_limit_bytes=mib * 1024 * 1024)


def cost(flops, moved):
    return pl.CostEstimate(flops=flops, bytes_accessed=moved, transcendentals=0)


def line_shift(n_expert, n_width, shift, second):
    side = int(round(n_expert**0.5))
    pairs = []
    for e in range(n_expert):
        y, z = e // side, e % side
        for w in range(n_width):
            if (w % 2 == 0) != second:
                to = ((y + shift) % side) * side + z
            else:
                to = y * side + (z + shift) % side
            pairs.append((e * n_width + w, to * n_width + w))
    return pairs


def here():
    n_expert = lax.axis_size("expert")
    side = int(round(n_expert**0.5))
    me = lax.axis_index("expert")
    return side, lax.div(me, side), lax.rem(me, side), lax.rem(lax.axis_index("width"), 2)


def cell(place, along, across):
    side, y, z, core = place
    along, across = along % side, across % side
    first = lax.rem(y + along, side) * side + lax.rem(z + across, side)
    second = lax.rem(y + across, side) * side + lax.rem(z + along, side)
    return jnp.where(core == 0, first, second)


def in_hbm(x):
    return pltpu.with_memory_space_constraint(x, pltpu.HBM)


def pack_kernel(per_device, x_ref, ids_ref, slots_ref, out_ref, held_ids, held_slots, sem):
    tok, width = x_ref.shape
    top = ids_ref.shape[0]
    copies = [
        pltpu.make_async_copy(ids_ref, held_ids, sem.at[0]),
        pltpu.make_async_copy(slots_ref, held_slots, sem.at[1]),
        pltpu.make_async_copy(x_ref, out_ref.at[pl.ds(0, tok), :], sem.at[2]),
    ]
    for copy in copies:
        copy.start()
    copies[0].wait()
    copies[1].wait()
    dev = (held_ids[...] // per_device).astype(f32)
    slots = held_slots[...].astype(f32)
    rest = jnp.zeros((top, width - 2 * tok), f32)
    out_ref[tok:, :] = jnp.concatenate([dev, slots, rest], axis=1).astype(bf16)
    copies[2].wait()


def compact_kernel(parts, tok, cap, n_dest, halves, *refs):
    n_in, n_half = sum(parts), len(halves)
    x_refs, (stage, sem) = refs[:n_in], refs[-2:]
    out_refs, half_refs = refs[-2 - n_half - n_dest : -2 - n_half], refs[-2 - n_half : -2]
    place = here()
    copies = []
    for at, (j, rows, first) in enumerate(halves):
        part = x_refs[j].at[pl.ds(first, rows), :]
        copies.append(pltpu.make_async_copy(part, half_refs[at], sem.at[n_dest + at]))
        copies[-1].start()
    for d in list(range(1, n_dest)) + [0]:
        at = 0
        for j, count in enumerate(parts):
            mine_refs = x_refs[at : at + count]
            at += count
            last = mine_refs[-1].shape[0]
            top = sum(ref.shape[0] for ref in mine_refs) - tok
            info = mine_refs[-1][last - top :, :].astype(f32)
            dev, slots = info[:, :tok], info[:, tok : 2 * tok]
            mine = dev == cell(place, 0, d).astype(f32)
            slot = jnp.sum(jnp.where(mine, slots + 1.0, 0.0), axis=0, keepdims=True).astype(i32) - 1
            got, first = None, 0
            for ref in mine_refs:
                rows = min(ref.shape[0], tok - first)
                want = lax.broadcasted_iota(i32, (cap, rows), 0)
                table = jnp.where(want == slot[:, first : first + rows], 1.0, 0.0).astype(bf16)
                term = jnp.dot(table, ref[:rows, :], preferred_element_type=f32)
                got = term if got is None else got + term
                first += rows
            stage[d, j * cap : (j + 1) * cap, :] = got.astype(bf16)
        copies.append(pltpu.make_async_copy(stage.at[d], out_refs[d], sem.at[d]))
        copies[-1].start()
    for copy in copies:
        copy.wait()


def compact(sources, after, tok, cap, n_dest, halves=()):
    n_src, width = len(sources), sources[0][0].shape[1]
    xs = sum(sources, [])
    outs = [pltpu.HBM((n_src * cap, width), bf16)] * n_dest
    outs += [pltpu.HBM((rows, width), bf16) for _, rows, _ in halves]
    return pl.pallas_call(
        functools.partial(compact_kernel, [len(x) for x in sources], tok, cap, n_dest, halves),
        out_shape=outs,
        in_specs=[VMEM] * len(xs) + [HBM] * len(after),
        out_specs=[HBM] * len(outs),
        scratch_shapes=[
            pltpu.VMEM((n_dest, n_src * cap, width), bf16),
            pltpu.SemaphoreType.DMA((n_dest + len(halves),)),
        ],
        compiler_params=params(12),
        cost_estimate=cost(2 * n_src * n_dest * cap * tok * width, n_src * tok * width * 6),
        name="compact",
    )(*xs, *map(in_hbm, after))


def picked_kernel(ids_ref, tok_ref, w_ref, out_ref, ids, toks, weights, sem):
    copies = [
        pltpu.make_async_copy(w_ref, weights, sem.at[0]),
        pltpu.make_async_copy(tok_ref, toks, sem.at[1]),
        pltpu.make_async_copy(ids_ref, ids, sem.at[2]),
    ]
    for copy in copies:
        copy.start()
    for copy in copies:
        copy.wait()
    logits = lax.dot_general(
        weights[...], toks[...], (((0,), (1,)), ((), ())), preferred_element_type=f32
    )
    experts = lax.broadcasted_iota(i32, logits.shape, 0)
    rows = []
    for k in range(ids.shape[0]):
        hit = experts == ids[k : k + 1, :]
        rows.append(jnp.sum(jnp.where(hit, logits, 0.0), axis=0, keepdims=True))
    picked = jnp.concatenate(rows, axis=0)
    for w in range(out_ref.shape[0]):
        out_ref[w] = picked


def front(ids, tokens_in, router_weight, n_width):
    (top, tok), width, experts = ids.shape, tokens_in.shape[1], router_weight.shape[1]
    return pl.pallas_call(
        picked_kernel,
        out_shape=jax.ShapeDtypeStruct((n_width, top, tok), f32),
        in_specs=[HBM] * 3,
        out_specs=VMEM,
        scratch_shapes=[
            pltpu.VMEM((top, tok), i32),
            pltpu.VMEM((tok, width), bf16),
            pltpu.VMEM((width, experts), bf16),
            pltpu.SemaphoreType.DMA((3,)),
        ],
        compiler_params=params(6),
        cost_estimate=cost(2 * tok * width * experts, 2 * tok * width),
        name="picked",
    )(in_hbm(ids), in_hbm(tokens_in), in_hbm(router_weight))


def gates_of(parts):
    logits = jnp.sum(parts, axis=0)
    picked = 1.0 / (1.0 + jnp.exp(-logits))
    totals = jnp.sum(picked, axis=0, keepdims=True)
    return picked, totals


def gate_kernel(per_device, parts_ref, ids_ref, slots_ref, out_ref):
    picked, totals = gates_of(parts_ref[...])
    gates = (route_scale * picked / totals).astype(bf16).astype(f32)
    top, tok = ids_ref.shape
    n_expert, cap = out_ref.shape
    dev, slots = ids_ref[...] // per_device, slots_ref[...]
    dev_rows = lax.broadcasted_iota(i32, (n_expert, tok), 0)
    slot_rows = lax.broadcasted_iota(i32, (cap, tok), 0)
    total = jnp.zeros((n_expert, cap), f32)
    for k in range(top):
        left = jnp.where(dev_rows == dev[k : k + 1], gates[k : k + 1], 0.0).astype(bf16)
        right = jnp.where(slot_rows == slots[k : k + 1], 1.0, 0.0).astype(bf16)
        total = total + lax.dot_general(left, right, (((1,), (1,)), ((), ())), preferred_element_type=f32)
    out_ref[...] = total


def row_dots(chunk, other):
    total = None
    for at in range(0, chunk.shape[1], 128):
        term = chunk[:, at : at + 128].astype(f32) * other[:, at : at + 128].astype(f32)
        total = term if total is None else total + term
    return jnp.sum(total.T, axis=0, keepdims=True)


def fetch(eo_ref, stage, sem, cells, cap):
    copies = []
    for at, src in enumerate(cells):
        rows = eo_ref.at[pl.ds(pl.multiple_of(src * cap, cap), cap), :]
        copies.append(pltpu.make_async_copy(rows, stage.at[at], sem.at[at]))
        copies[-1].start()
    return copies


def fetch_chunks(chunk_refs, stage, sem, cap, first=0):
    copies, at = [], first
    for chunk_ref in chunk_refs:
        for j in range(chunk_ref.shape[0] // cap):
            copies.append(pltpu.make_async_copy(chunk_ref.at[pl.ds(j * cap, cap), :], stage.at[at], sem.at[at]))
            copies[-1].start()
            at += 1
    return copies


def cells_of(batch, side, place):
    return [cell(place, -s, -d) for d in range(side) for s in batch]


def dots_kernel(batch, side, cap, next_batch, eo_ref, *refs):
    chunk_refs = refs[:side]
    out_refs, (held, stage, sem, next_sem) = refs[side:-4], refs[-4:]
    place = here()
    rows = fetch_chunks(chunk_refs, held, sem.at[0], cap)
    others = fetch(eo_ref, stage, sem.at[1], cells_of(batch, side, place), cap)
    ahead = fetch(eo_ref, out_refs[1], next_sem, cells_of(next_batch, side, place), cap) if next_batch else []
    for at in range(len(rows)):
        rows[at].wait()
        others[at].wait()
        out_refs[0][at : at + 1, :] = row_dots(held.at[at], stage.at[at])
    for copy in ahead:
        copy.wait()


def row_dots_call(batch, next_batch, eo, chunks, cap):
    n, width, side = len(batch) * len(chunks), chunks[0].shape[1], len(chunks)
    n_next = len(next_batch) * side
    outs = [jax.ShapeDtypeStruct((n, cap), f32)]
    if n_next:
        outs.append(pltpu.VMEM((n_next, cap, width), bf16))
    return pl.pallas_call(
        functools.partial(dots_kernel, batch, side, cap, next_batch),
        out_shape=outs,
        in_specs=[HBM] * (1 + side),
        out_specs=[VMEM] * len(outs),
        scratch_shapes=[
            pltpu.VMEM((n, cap, width), bf16),
            pltpu.VMEM((n, cap, width), bf16),
            pltpu.SemaphoreType.DMA((2, n)),
            pltpu.SemaphoreType.DMA((max(n_next, 1),)),
        ],
        compiler_params=params(12),
        cost_estimate=cost(2 * n * cap * width, 4 * n * cap * width),
        name="dots",
    )(in_hbm(eo), *map(in_hbm, chunks))


def last_dots_kernel(n_width, batches, cap, side, gate_ref, eo_ref, *refs):
    chunk_refs, early_refs, (out_ref, held, sem) = refs[:side], refs[side:-3], refs[-3:]
    n_expert = gate_ref.shape[0]
    place = here()
    copies = fetch_chunks(chunk_refs, held, sem, cap)
    for e in range(n_expert):
        for w in range(n_width):
            out_ref[2 * (e * n_width + w) + 1] = gate_ref[e : e + 1, :]

    def put(src, row):
        base = src * (2 * n_width)
        for w in range(n_width):
            out_ref[base + 2 * w] = row

    for batch, early in zip(batches[:-1], early_refs):
        for at, src in enumerate(cells_of(batch, side, place)):
            put(src, early[at : at + 1, :])
    for at, src in enumerate(cells_of(batches[-1], side, place)):
        copies[at].wait()
        put(src, row_dots(held.at[at], eo_ref.at[at]))


def tail_kernel(n_expert, n_width, per_device, got_ref, parts_ref, ids_ref, slots_ref, tok_ref, lg_ref, router_ref):
    top, tok = ids_ref.shape
    rows = []
    for e in range(n_expert):
        row = got_ref[2 * e * n_width]
        for w in range(1, n_width):
            row = row + got_ref[2 * (e * n_width + w)]
        rows.append(row)
    dots = jnp.concatenate(rows, axis=0)
    cap = dots.shape[1]
    high = dots.astype(bf16)
    low = (dots - high.astype(f32)).astype(bf16)
    both = jnp.concatenate([high, low], axis=0)
    ids, slots = ids_ref[...], slots_ref[...]
    dev = ids // per_device
    slot_rows = lax.broadcasted_iota(i32, (cap, tok), 0)
    dev_rows = lax.broadcasted_iota(i32, (n_expert, tok), 0)
    out = []
    for k in range(top):
        table = jnp.where(slot_rows == slots[k : k + 1], 1.0, 0.0).astype(bf16)
        found = jnp.dot(both, table, preferred_element_type=f32)
        found = found[:n_expert] + found[n_expert:]
        out.append(jnp.sum(jnp.where(dev_rows == dev[k : k + 1], found, 0.0), axis=0, keepdims=True))
    gate_grads = jnp.concatenate(out, axis=0)
    picked, totals = gates_of(parts_ref[...])
    weighted = jnp.sum(gate_grads * picked, axis=0, keepdims=True) / totals
    local = route_scale / totals * (gate_grads - weighted) * picked * (1.0 - picked)
    experts = lax.broadcasted_iota(i32, (lg_ref.shape[0], tok), 0)
    grads = jnp.zeros(lg_ref.shape, f32)
    for k in range(top):
        grads = grads + jnp.where(experts == ids[k : k + 1], local[k : k + 1], 0.0)
    grads = grads.astype(bf16)
    lg_ref[...] = grads
    router_ref[...] = jnp.dot(grads, tok_ref[...], preferred_element_type=f32).astype(bf16)


def scale_kernel(n_width, batches, cap, side, got_ref, lg_ref, w_ref, *refs):
    chunk_refs, (out_ref, input_ref, held, stage, in_sem, sem) = refs[:-6], refs[-6:]
    place = here()
    rows = fetch_chunks(chunk_refs, held, in_sem, cap)
    copies = []
    cells = sum([cells_of(batch, side, place) for batch in batches], [])
    for at, src in enumerate(cells):
        gate = jnp.broadcast_to(got_ref[src * (2 * n_width) + 1], (128, cap)).T
        rows[at].wait()
        for lane in range(0, held.shape[2], 128):
            part = held[at, :, lane : lane + 128].astype(f32)
            stage[at, :, lane : lane + 128] = (part * gate).astype(bf16)
        to = out_ref.at[pl.ds(pl.multiple_of(src * cap, cap), cap), :]
        copies.append(pltpu.make_async_copy(stage.at[at], to, sem.at[at]))
        copies[-1].start()
    input_ref[...] = lax.dot_general(
        lg_ref[...], w_ref[...], (((0,), (1,)), ((), ())), preferred_element_type=f32
    ).astype(bf16)
    for copy in copies:
        copy.wait()


def body(tokens_in, out_grad, router_weight, expert_out, expert_ids, slot_ids):
    n_expert, n_width = lax.axis_size("expert"), lax.axis_size("width")
    side = int(round(n_expert**0.5))
    tok, width = out_grad.shape
    top = expert_ids.shape[1]
    experts = router_weight.shape[1]
    per_device = experts // n_expert
    cap = tok * top // n_expert

    def send(x, shift, second):
        return lax.ppermute(x, AXES, line_shift(n_expert, n_width, shift, second))

    ids, slots = expert_ids.T, slot_ids.T
    packed = pl.pallas_call(
        functools.partial(pack_kernel, per_device),
        out_shape=jax.ShapeDtypeStruct((tok + top, width), bf16),
        in_specs=[HBM] * 3,
        out_specs=VMEM,
        scratch_shapes=[
            pltpu.VMEM((top, tok), i32),
            pltpu.VMEM((top, tok), i32),
            pltpu.SemaphoreType.DMA((3,)),
        ],
        compiler_params=params(4),
        cost_estimate=cost(0, 4 * tok * width),
        name="pack",
    )(in_hbm(out_grad), in_hbm(ids), in_hbm(slots))
    xs = {0: packed}
    for s in [1, side - 1] + list(range(2, side - 1)):
        xs[s] = send(packed, s, False)
    batches = [[0, 1, side - 1], list(range(2, side - 1))]

    sent_parts = front(ids, tokens_in, router_weight, n_width)
    parts = lax.all_to_all(sent_parts, "width", 0, 0, tiled=True)

    landed, after = [], []
    for batch in batches:
        chunks = compact([[xs[s]] for s in batch], after, tok, cap, side)
        after = [chunks[0]]
        group = [chunks[0]]
        for d in range(1, side):
            group.append(send(chunks[d], d, True))
        landed.append(group)

    gates = pl.pallas_call(
        functools.partial(gate_kernel, per_device),
        out_shape=jax.ShapeDtypeStruct((n_expert, cap), f32),
        in_specs=[VMEM] * 3,
        out_specs=VMEM,
        compiler_params=params(4),
        cost_estimate=cost(2 * top * n_expert * cap * tok, 4 * n_width * top * tok),
        name="gates",
    )(parts, ids, slots)

    early = []
    for b, batch in enumerate(batches[:-1]):
        next_batch = batches[-1] if b == len(batches) - 2 else []
        outs = row_dots_call(batch, next_batch, expert_out, landed[b], cap)
        early.append(outs[0])
    sent = pl.pallas_call(
        functools.partial(last_dots_kernel, n_width, batches, cap, side),
        out_shape=jax.ShapeDtypeStruct((2 * n_expert * n_width, 1, cap), f32),
        in_specs=[VMEM] * 2 + [HBM] * side + [VMEM] * len(early),
        out_specs=VMEM,
        scratch_shapes=[
            pltpu.VMEM((side, cap, width), bf16),
            pltpu.SemaphoreType.DMA((side,)),
        ],
        compiler_params=params(6),
        cost_estimate=cost(2 * side * cap * width, 4 * side * cap * width),
        name="last_dots",
    )(gates, outs[1], *map(in_hbm, landed[-1]), *early)
    got = lax.all_to_all(sent, AXES, 0, 0, tiled=True)

    logit_grads, router_part = pl.pallas_call(
        functools.partial(tail_kernel, n_expert, n_width, per_device),
        out_shape=[
            jax.ShapeDtypeStruct((experts, tok), bf16),
            jax.ShapeDtypeStruct((experts, width), bf16),
        ],
        in_specs=[VMEM] * 5,
        out_specs=[VMEM] * 2,
        compiler_params=params(8),
        cost_estimate=cost(2 * tok * width * experts, 2 * tok * width),
        name="tail",
    )(got, parts, ids, slots, tokens_in)
    blocks = lax.all_to_all(router_part.reshape(n_expert, per_device, width), "expert", 0, 0, tiled=True)
    flat = sum(landed, [])
    expert_grad, input_grad = pl.pallas_call(
        functools.partial(scale_kernel, n_width, batches, cap, side),
        out_shape=[
            jax.ShapeDtypeStruct(expert_out.shape, bf16),
            jax.ShapeDtypeStruct((tok, width), bf16),
        ],
        in_specs=[VMEM] * 3 + [HBM] * len(flat),
        out_specs=[HBM, VMEM],
        scratch_shapes=[
            pltpu.VMEM((n_expert, cap, width), bf16),
            pltpu.VMEM((n_expert, cap, width), bf16),
            pltpu.SemaphoreType.DMA((n_expert,)),
            pltpu.SemaphoreType.DMA((n_expert,)),
        ],
        compiler_params=params(16),
        cost_estimate=cost(2 * tok * width * experts, 4 * n_expert * cap * width),
        name="scale",
    )(got, logit_grads, router_weight, *map(in_hbm, flat))
    router_grad = jnp.sum(blocks.astype(f32), axis=0).T
    return (expert_grad, router_grad, input_grad)


def solution(mesh):
    return jax.shard_map(
        body,
        mesh=mesh,
        in_specs=(
            P("expert", "width"),
            P("expert", "width"),
            P("width", None),
            P("expert", "width"),
            P("expert", None),
            P("expert", None),
        ),
        out_specs=(P("expert", "width"), P("width", "expert"), P("expert", "width")),
        check_vma=False,
    )
```

```python
import functools

import jax
import jax.numpy as jnp
from jax import lax
from jax.experimental import pallas as pl
from jax.experimental.pallas import tpu as pltpu
from jax.sharding import PartitionSpec as P


route_scale = 2.5
AXES = ("expert", "width")
f32, bf16, i32 = jnp.float32, jnp.bfloat16, jnp.int32
VMEM = pl.BlockSpec(memory_space=pltpu.VMEM)
SMEM = pl.BlockSpec(memory_space=pltpu.SMEM)
ANY = pl.BlockSpec(memory_space=pl.ANY)
HBM = pl.BlockSpec(memory_space=pltpu.HBM)


def params(mib):
    return pltpu.CompilerParams(vmem_limit_bytes=mib * 1024 * 1024)


def cost(flops, moved):
    return pl.CostEstimate(flops=flops, bytes_accessed=moved, transcendentals=0)


def line_shift(n_expert, n_width, shift, second):
    side = int(round(n_expert**0.5))
    pairs = []
    for e in range(n_expert):
        y, z = e // side, e % side
        for w in range(n_width):
            if (w % 2 == 0) != second:
                to = ((y + shift) % side) * side + z
            else:
                to = y * side + (z + shift) % side
            pairs.append((e * n_width + w, to * n_width + w))
    return pairs


def here():
    n_expert = lax.axis_size("expert")
    side = int(round(n_expert**0.5))
    me = lax.axis_index("expert")
    return side, lax.div(me, side), lax.rem(me, side), lax.rem(lax.axis_index("width"), 2)


def cell(place, along, across):
    side, y, z, core = place
    along, across = along % side, across % side
    first = lax.rem(y + along, side) * side + lax.rem(z + across, side)
    second = lax.rem(y + across, side) * side + lax.rem(z + along, side)
    return jnp.where(core == 0, first, second)


def in_hbm(x):
    return pltpu.with_memory_space_constraint(x, pltpu.HBM)


def pack_kernel(per_device, x_ref, ids_ref, slots_ref, out_ref, held_ids, held_slots, sem):
    tok, width = x_ref.shape
    top = ids_ref.shape[0]
    copies = [
        pltpu.make_async_copy(ids_ref, held_ids, sem.at[0]),
        pltpu.make_async_copy(slots_ref, held_slots, sem.at[1]),
        pltpu.make_async_copy(x_ref, out_ref.at[pl.ds(0, tok), :], sem.at[2]),
    ]
    for copy in copies:
        copy.start()
    copies[0].wait()
    copies[1].wait()
    dev = (held_ids[...] // per_device).astype(f32)
    slots = held_slots[...].astype(f32)
    rest = jnp.zeros((top, width - 2 * tok), f32)
    out_ref[tok:, :] = jnp.concatenate([dev, slots, rest], axis=1).astype(bf16)
    copies[2].wait()


def compact_kernel(parts, tok, cap, n_dest, halves, *refs):
    n_in, n_half = sum(parts), len(halves)
    x_refs, (stage, sem) = refs[:n_in], refs[-2:]
    out_refs, half_refs = refs[-2 - n_half - n_dest : -2 - n_half], refs[-2 - n_half : -2]
    place = here()
    copies = []
    for at, (j, rows, first) in enumerate(halves):
        part = x_refs[j].at[pl.ds(first, rows), :]
        copies.append(pltpu.make_async_copy(part, half_refs[at], sem.at[n_dest + at]))
        copies[-1].start()
    for d in list(range(1, n_dest)) + [0]:
        at = 0
        for j, count in enumerate(parts):
            mine_refs = x_refs[at : at + count]
            at += count
            last = mine_refs[-1].shape[0]
            top = sum(ref.shape[0] for ref in mine_refs) - tok
            info = mine_refs[-1][last - top :, :].astype(f32)
            dev, slots = info[:, :tok], info[:, tok : 2 * tok]
            mine = dev == cell(place, 0, d).astype(f32)
            slot = jnp.sum(jnp.where(mine, slots + 1.0, 0.0), axis=0, keepdims=True).astype(i32) - 1
            got, first = None, 0
            for ref in mine_refs:
                rows = min(ref.shape[0], tok - first)
                want = lax.broadcasted_iota(i32, (cap, rows), 0)
                table = jnp.where(want == slot[:, first : first + rows], 1.0, 0.0).astype(bf16)
                term = jnp.dot(table, ref[:rows, :], preferred_element_type=f32)
                got = term if got is None else got + term
                first += rows
            stage[d, j * cap : (j + 1) * cap, :] = got.astype(bf16)
        copies.append(pltpu.make_async_copy(stage.at[d], out_refs[d], sem.at[d]))
        copies[-1].start()
    for copy in copies:
        copy.wait()


def compact(sources, after, tok, cap, n_dest, halves=()):
    n_src, width = len(sources), sources[0][0].shape[1]
    xs = sum(sources, [])
    outs = [pltpu.HBM((n_src * cap, width), bf16)] * n_dest
    outs += [pltpu.HBM((rows, width), bf16) for _, rows, _ in halves]
    return pl.pallas_call(
        functools.partial(compact_kernel, [len(x) for x in sources], tok, cap, n_dest, halves),
        out_shape=outs,
        in_specs=[VMEM] * len(xs) + [HBM] * len(after),
        out_specs=[HBM] * len(outs),
        scratch_shapes=[
            pltpu.VMEM((n_dest, n_src * cap, width), bf16),
            pltpu.SemaphoreType.DMA((n_dest + len(halves),)),
        ],
        compiler_params=params(12),
        cost_estimate=cost(2 * n_src * n_dest * cap * tok * width, n_src * tok * width * 6),
        name="compact",
    )(*xs, *map(in_hbm, after))


def picked_kernel(ids_ref, tok_ref, w_ref, out_ref, ids, toks, weights, sem):
    copies = [
        pltpu.make_async_copy(w_ref, weights, sem.at[0]),
        pltpu.make_async_copy(tok_ref, toks, sem.at[1]),
        pltpu.make_async_copy(ids_ref, ids, sem.at[2]),
    ]
    for copy in copies:
        copy.start()
    for copy in copies:
        copy.wait()
    logits = lax.dot_general(
        weights[...], toks[...], (((0,), (1,)), ((), ())), preferred_element_type=f32
    )
    experts = lax.broadcasted_iota(i32, logits.shape, 0)
    rows = []
    for k in range(ids.shape[0]):
        hit = experts == ids[k : k + 1, :]
        rows.append(jnp.sum(jnp.where(hit, logits, 0.0), axis=0, keepdims=True))
    picked = jnp.concatenate(rows, axis=0)
    for w in range(out_ref.shape[0]):
        out_ref[w] = picked


def front(ids, tokens_in, router_weight, n_width):
    (top, tok), width, experts = ids.shape, tokens_in.shape[1], router_weight.shape[1]
    return pl.pallas_call(
        picked_kernel,
        out_shape=jax.ShapeDtypeStruct((n_width, top, tok), f32),
        in_specs=[HBM] * 3,
        out_specs=VMEM,
        scratch_shapes=[
            pltpu.VMEM((top, tok), i32),
            pltpu.VMEM((tok, width), bf16),
            pltpu.VMEM((width, experts), bf16),
            pltpu.SemaphoreType.DMA((3,)),
        ],
        compiler_params=params(6),
        cost_estimate=cost(2 * tok * width * experts, 2 * tok * width),
        name="picked",
    )(in_hbm(ids), in_hbm(tokens_in), in_hbm(router_weight))


def gates_of(parts):
    logits = jnp.sum(parts, axis=0)
    picked = 1.0 / (1.0 + jnp.exp(-logits))
    totals = jnp.sum(picked, axis=0, keepdims=True)
    return picked, totals


def gate_kernel(per_device, parts_ref, ids_ref, slots_ref, out_ref):
    picked, totals = gates_of(parts_ref[...])
    gates = (route_scale * picked / totals).astype(bf16).astype(f32)
    top, tok = ids_ref.shape
    n_expert, cap = out_ref.shape
    dev, slots = ids_ref[...] // per_device, slots_ref[...]
    dev_rows = lax.broadcasted_iota(i32, (n_expert, tok), 0)
    slot_rows = lax.broadcasted_iota(i32, (cap, tok), 0)
    total = jnp.zeros((n_expert, cap), f32)
    for k in range(top):
        left = jnp.where(dev_rows == dev[k : k + 1], gates[k : k + 1], 0.0).astype(bf16)
        right = jnp.where(slot_rows == slots[k : k + 1], 1.0, 0.0).astype(bf16)
        total = total + lax.dot_general(left, right, (((1,), (1,)), ((), ())), preferred_element_type=f32)
    out_ref[...] = total


def row_dots(chunk, other):
    total = None
    for at in range(0, chunk.shape[1], 128):
        term = chunk[:, at : at + 128].astype(f32) * other[:, at : at + 128].astype(f32)
        total = term if total is None else total + term
    return jnp.sum(total.T, axis=0, keepdims=True)


def fetch(eo_ref, stage, sem, cells, cap):
    copies = []
    for at, src in enumerate(cells):
        rows = eo_ref.at[pl.ds(pl.multiple_of(src * cap, cap), cap), :]
        copies.append(pltpu.make_async_copy(rows, stage.at[at], sem.at[at]))
        copies[-1].start()
    return copies


def fetch_chunks(chunk_refs, stage, sem, cap, first=0):
    copies, at = [], first
    for chunk_ref in chunk_refs:
        for j in range(chunk_ref.shape[0] // cap):
            copies.append(pltpu.make_async_copy(chunk_ref.at[pl.ds(j * cap, cap), :], stage.at[at], sem.at[at]))
            copies[-1].start()
            at += 1
    return copies


def cells_of(batch, side, place):
    return [cell(place, -s, -d) for d in range(side) for s in batch]


def dots_kernel(batch, side, cap, next_batch, eo_ref, *refs):
    chunk_refs = refs[:side]
    out_refs, (held, stage, sem, next_sem) = refs[side:-4], refs[-4:]
    place = here()
    rows = fetch_chunks(chunk_refs, held, sem.at[0], cap)
    others = fetch(eo_ref, stage, sem.at[1], cells_of(batch, side, place), cap)
    ahead = fetch(eo_ref, out_refs[1], next_sem, cells_of(next_batch, side, place), cap) if next_batch else []
    for at in range(len(rows)):
        rows[at].wait()
        others[at].wait()
        out_refs[0][at : at + 1, :] = row_dots(held.at[at], stage.at[at])
    for copy in ahead:
        copy.wait()


def row_dots_call(batch, next_batch, eo, chunks, cap):
    n, width, side = len(batch) * len(chunks), chunks[0].shape[1], len(chunks)
    n_next = len(next_batch) * side
    outs = [jax.ShapeDtypeStruct((n, cap), f32)]
    if n_next:
        outs.append(pltpu.VMEM((n_next, cap, width), bf16))
    return pl.pallas_call(
        functools.partial(dots_kernel, batch, side, cap, next_batch),
        out_shape=outs,
        in_specs=[HBM] * (1 + side),
        out_specs=[VMEM] * len(outs),
        scratch_shapes=[
            pltpu.VMEM((n, cap, width), bf16),
            pltpu.VMEM((n, cap, width), bf16),
            pltpu.SemaphoreType.DMA((2, n)),
            pltpu.SemaphoreType.DMA((max(n_next, 1),)),
        ],
        compiler_params=params(12),
        cost_estimate=cost(2 * n * cap * width, 4 * n * cap * width),
        name="dots",
    )(in_hbm(eo), *map(in_hbm, chunks))


def last_dots_kernel(n_width, batches, side, gate_ref, eo_ref, *refs):
    chunk_refs, early_refs, out_ref = refs[:side], refs[side:-1], refs[-1]
    n_expert = gate_ref.shape[0]
    place = here()
    for e in range(n_expert):
        for w in range(n_width):
            out_ref[2 * (e * n_width + w) + 1] = gate_ref[e : e + 1, :]

    def put(src, row):
        base = src * (2 * n_width)
        for w in range(n_width):
            out_ref[base + 2 * w] = row

    for batch, early in zip(batches[:-1], early_refs):
        for at, src in enumerate(cells_of(batch, side, place)):
            put(src, early[at : at + 1, :])
    for at, src in enumerate(cells_of(batches[-1], side, place)):
        put(src, row_dots(chunk_refs[at], eo_ref.at[at]))


def tail_kernel(n_expert, n_width, per_device, got_ref, parts_ref, ids_ref, slots_ref, tok_ref, lg_ref, router_ref):
    top, tok = ids_ref.shape
    rows = []
    for e in range(n_expert):
        row = got_ref[2 * e * n_width]
        for w in range(1, n_width):
            row = row + got_ref[2 * (e * n_width + w)]
        rows.append(row)
    dots = jnp.concatenate(rows, axis=0)
    cap = dots.shape[1]
    high = dots.astype(bf16)
    low = (dots - high.astype(f32)).astype(bf16)
    both = jnp.concatenate([high, low], axis=0)
    ids, slots = ids_ref[...], slots_ref[...]
    dev = ids // per_device
    slot_rows = lax.broadcasted_iota(i32, (cap, tok), 0)
    dev_rows = lax.broadcasted_iota(i32, (n_expert, tok), 0)
    out = []
    for k in range(top):
        table = jnp.where(slot_rows == slots[k : k + 1], 1.0, 0.0).astype(bf16)
        found = jnp.dot(both, table, preferred_element_type=f32)
        found = found[:n_expert] + found[n_expert:]
        out.append(jnp.sum(jnp.where(dev_rows == dev[k : k + 1], found, 0.0), axis=0, keepdims=True))
    gate_grads = jnp.concatenate(out, axis=0)
    picked, totals = gates_of(parts_ref[...])
    weighted = jnp.sum(gate_grads * picked, axis=0, keepdims=True) / totals
    local = route_scale / totals * (gate_grads - weighted) * picked * (1.0 - picked)
    experts = lax.broadcasted_iota(i32, (lg_ref.shape[0], tok), 0)
    grads = jnp.zeros(lg_ref.shape, f32)
    for k in range(top):
        grads = grads + jnp.where(experts == ids[k : k + 1], local[k : k + 1], 0.0)
    grads = grads.astype(bf16)
    lg_ref[...] = grads
    router_ref[...] = jnp.dot(grads, tok_ref[...], preferred_element_type=f32).astype(bf16)


def scale_kernel(n_width, batches, cap, side, got_ref, lg_ref, w_ref, *refs):
    chunk_refs, (out_ref, input_ref, held, stage, in_sem, sem) = refs[:-6], refs[-6:]
    place = here()
    rows = fetch_chunks(chunk_refs, held, in_sem, cap)
    copies = []
    cells = sum([cells_of(batch, side, place) for batch in batches], [])
    for at, src in enumerate(cells):
        gate = jnp.broadcast_to(got_ref[src * (2 * n_width) + 1], (128, cap)).T
        rows[at].wait()
        for lane in range(0, held.shape[2], 128):
            part = held[at, :, lane : lane + 128].astype(f32)
            stage[at, :, lane : lane + 128] = (part * gate).astype(bf16)
        to = out_ref.at[pl.ds(pl.multiple_of(src * cap, cap), cap), :]
        copies.append(pltpu.make_async_copy(stage.at[at], to, sem.at[at]))
        copies[-1].start()
    input_ref[...] = lax.dot_general(
        lg_ref[...], w_ref[...], (((0,), (1,)), ((), ())), preferred_element_type=f32
    ).astype(bf16)
    for copy in copies:
        copy.wait()


def body(tokens_in, out_grad, router_weight, expert_out, expert_ids, slot_ids):
    n_expert, n_width = lax.axis_size("expert"), lax.axis_size("width")
    side = int(round(n_expert**0.5))
    tok, width = out_grad.shape
    top = expert_ids.shape[1]
    experts = router_weight.shape[1]
    per_device = experts // n_expert
    cap = tok * top // n_expert

    def send(x, shift, second):
        return lax.ppermute(x, AXES, line_shift(n_expert, n_width, shift, second))

    ids, slots = expert_ids.T, slot_ids.T
    packed = pl.pallas_call(
        functools.partial(pack_kernel, per_device),
        out_shape=jax.ShapeDtypeStruct((tok + top, width), bf16),
        in_specs=[HBM] * 3,
        out_specs=VMEM,
        scratch_shapes=[
            pltpu.VMEM((top, tok), i32),
            pltpu.VMEM((top, tok), i32),
            pltpu.SemaphoreType.DMA((3,)),
        ],
        compiler_params=params(4),
        cost_estimate=cost(0, 4 * tok * width),
        name="pack",
    )(in_hbm(out_grad), in_hbm(ids), in_hbm(slots))
    xs = {0: packed}
    for s in [1, side - 1] + list(range(2, side - 1)):
        xs[s] = send(packed, s, False)
    batches = [[0, 1, side - 1], list(range(2, side - 1))]

    sent_parts = front(ids, tokens_in, router_weight, n_width)
    parts = lax.all_to_all(sent_parts, "width", 0, 0, tiled=True)

    landed, after = [], []
    for batch in batches:
        chunks = compact([[xs[s]] for s in batch], after, tok, cap, side)
        after = [chunks[0]]
        group = [chunks[0]]
        for d in range(1, side):
            group.append(send(chunks[d], d, True))
        landed.append(group)

    gates = pl.pallas_call(
        functools.partial(gate_kernel, per_device),
        out_shape=jax.ShapeDtypeStruct((n_expert, cap), f32),
        in_specs=[VMEM] * 3,
        out_specs=VMEM,
        compiler_params=params(4),
        cost_estimate=cost(2 * top * n_expert * cap * tok, 4 * n_width * top * tok),
        name="gates",
    )(parts, ids, slots)

    early = []
    for b, batch in enumerate(batches[:-1]):
        next_batch = batches[-1] if b == len(batches) - 2 else []
        outs = row_dots_call(batch, next_batch, expert_out, landed[b], cap)
        early.append(outs[0])
    sent = pl.pallas_call(
        functools.partial(last_dots_kernel, n_width, batches, side),
        out_shape=jax.ShapeDtypeStruct((2 * n_expert * n_width, 1, cap), f32),
        in_specs=[VMEM] * (2 + side + len(early)),
        out_specs=VMEM,
        compiler_params=params(6),
        cost_estimate=cost(2 * side * cap * width, 4 * side * cap * width),
        name="last_dots",
    )(gates, outs[1], *landed[-1], *early)
    got = lax.all_to_all(sent, AXES, 0, 0, tiled=True)

    logit_grads, router_part = pl.pallas_call(
        functools.partial(tail_kernel, n_expert, n_width, per_device),
        out_shape=[
            jax.ShapeDtypeStruct((experts, tok), bf16),
            jax.ShapeDtypeStruct((experts, width), bf16),
        ],
        in_specs=[VMEM] * 5,
        out_specs=[VMEM] * 2,
        compiler_params=params(8),
        cost_estimate=cost(2 * tok * width * experts, 2 * tok * width),
        name="tail",
    )(got, parts, ids, slots, tokens_in)
    blocks = lax.all_to_all(router_part.reshape(n_expert, per_device, width), "expert", 0, 0, tiled=True)
    flat = sum(landed, [])
    expert_grad, input_grad = pl.pallas_call(
        functools.partial(scale_kernel, n_width, batches, cap, side),
        out_shape=[
            jax.ShapeDtypeStruct(expert_out.shape, bf16),
            jax.ShapeDtypeStruct((tok, width), bf16),
        ],
        in_specs=[VMEM] * 3 + [HBM] * len(flat),
        out_specs=[HBM, VMEM],
        scratch_shapes=[
            pltpu.VMEM((n_expert, cap, width), bf16),
            pltpu.VMEM((n_expert, cap, width), bf16),
            pltpu.SemaphoreType.DMA((n_expert,)),
            pltpu.SemaphoreType.DMA((n_expert,)),
        ],
        compiler_params=params(16),
        cost_estimate=cost(2 * tok * width * experts, 4 * n_expert * cap * width),
        name="scale",
    )(got, logit_grads, router_weight, *map(in_hbm, flat))
    router_grad = jnp.sum(blocks.astype(f32), axis=0).T
    return (expert_grad, router_grad, input_grad)


def solution(mesh):
    return jax.shard_map(
        body,
        mesh=mesh,
        in_specs=(
            P("expert", "width"),
            P("expert", "width"),
            P("width", None),
            P("expert", "width"),
            P("expert", None),
            P("expert", None),
        ),
        out_specs=(P("expert", "width"), P("width", "expert"), P("expert", "width")),
        check_vma=False,
    )
```

```python
import functools

import jax
import jax.numpy as jnp
from jax import lax
from jax.experimental import pallas as pl
from jax.experimental.pallas import tpu as pltpu
from jax.sharding import PartitionSpec as P


route_scale = 2.5
AXES = ("expert", "width")
f32, bf16, i32 = jnp.float32, jnp.bfloat16, jnp.int32
VMEM = pl.BlockSpec(memory_space=pltpu.VMEM)
SMEM = pl.BlockSpec(memory_space=pltpu.SMEM)
ANY = pl.BlockSpec(memory_space=pl.ANY)
HBM = pl.BlockSpec(memory_space=pltpu.HBM)


def params(mib):
    return pltpu.CompilerParams(vmem_limit_bytes=mib * 1024 * 1024)


def cost(flops, moved):
    return pl.CostEstimate(flops=flops, bytes_accessed=moved, transcendentals=0)


def line_shift(n_expert, n_width, shift, second):
    side = int(round(n_expert**0.5))
    pairs = []
    for e in range(n_expert):
        y, z = e // side, e % side
        for w in range(n_width):
            if (w % 2 == 0) != second:
                to = ((y + shift) % side) * side + z
            else:
                to = y * side + (z + shift) % side
            pairs.append((e * n_width + w, to * n_width + w))
    return pairs


def here():
    n_expert = lax.axis_size("expert")
    side = int(round(n_expert**0.5))
    me = lax.axis_index("expert")
    return side, lax.div(me, side), lax.rem(me, side), lax.rem(lax.axis_index("width"), 2)


def cell(place, along, across):
    side, y, z, core = place
    along, across = along % side, across % side
    first = lax.rem(y + along, side) * side + lax.rem(z + across, side)
    second = lax.rem(y + across, side) * side + lax.rem(z + along, side)
    return jnp.where(core == 0, first, second)


def in_hbm(x):
    return pltpu.with_memory_space_constraint(x, pltpu.HBM)


def pack_kernel(per_device, x_ref, ids_ref, slots_ref, first_ref, last_ref, held_ids, held_slots, sem):
    tok, width = x_ref.shape
    top, half = ids_ref.shape[0], first_ref.shape[0]
    copies = [
        pltpu.make_async_copy(ids_ref, held_ids, sem.at[0]),
        pltpu.make_async_copy(slots_ref, held_slots, sem.at[1]),
        pltpu.make_async_copy(x_ref.at[pl.ds(0, half), :], first_ref, sem.at[2]),
        pltpu.make_async_copy(x_ref.at[pl.ds(half, tok - half), :], last_ref.at[pl.ds(0, tok - half), :], sem.at[3]),
    ]
    for copy in copies:
        copy.start()
    copies[0].wait()
    copies[1].wait()
    dev = (held_ids[...] // per_device).astype(f32)
    slots = held_slots[...].astype(f32)
    rest = jnp.zeros((top, width - 2 * tok), f32)
    last_ref[tok - half :, :] = jnp.concatenate([dev, slots, rest], axis=1).astype(bf16)
    copies[2].wait()
    copies[3].wait()


def compact_kernel(parts, tok, cap, n_dest, halves, *refs):
    n_in, n_half = sum(parts), len(halves)
    x_refs, (stage, sem) = refs[:n_in], refs[-2:]
    out_refs, half_refs = refs[-2 - n_half - n_dest : -2 - n_half], refs[-2 - n_half : -2]
    place = here()
    copies = []
    for at, (j, rows, first) in enumerate(halves):
        part = x_refs[j].at[pl.ds(first, rows), :]
        copies.append(pltpu.make_async_copy(part, half_refs[at], sem.at[n_dest + at]))
        copies[-1].start()
    for d in list(range(1, n_dest)) + [0]:
        at = 0
        for j, count in enumerate(parts):
            mine_refs = x_refs[at : at + count]
            at += count
            last = mine_refs[-1].shape[0]
            top = sum(ref.shape[0] for ref in mine_refs) - tok
            info = mine_refs[-1][last - top :, :].astype(f32)
            dev, slots = info[:, :tok], info[:, tok : 2 * tok]
            mine = dev == cell(place, 0, d).astype(f32)
            slot = jnp.sum(jnp.where(mine, slots + 1.0, 0.0), axis=0, keepdims=True).astype(i32) - 1
            got, first = None, 0
            for ref in mine_refs:
                rows = min(ref.shape[0], tok - first)
                want = lax.broadcasted_iota(i32, (cap, rows), 0)
                table = jnp.where(want == slot[:, first : first + rows], 1.0, 0.0).astype(bf16)
                term = jnp.dot(table, ref[:rows, :], preferred_element_type=f32)
                got = term if got is None else got + term
                first += rows
            stage[d, j * cap : (j + 1) * cap, :] = got.astype(bf16)
        copies.append(pltpu.make_async_copy(stage.at[d], out_refs[d], sem.at[d]))
        copies[-1].start()
    for copy in copies:
        copy.wait()


def compact(sources, after, tok, cap, n_dest, halves=()):
    n_src, width = len(sources), sources[0][0].shape[1]
    xs = sum(sources, [])
    outs = [pltpu.HBM((n_src * cap, width), bf16)] * n_dest
    outs += [pltpu.HBM((rows, width), bf16) for _, rows, _ in halves]
    return pl.pallas_call(
        functools.partial(compact_kernel, [len(x) for x in sources], tok, cap, n_dest, halves),
        out_shape=outs,
        in_specs=[VMEM] * len(xs) + [HBM] * len(after),
        out_specs=[HBM] * len(outs),
        scratch_shapes=[
            pltpu.VMEM((n_dest, n_src * cap, width), bf16),
            pltpu.SemaphoreType.DMA((n_dest + len(halves),)),
        ],
        compiler_params=params(12),
        cost_estimate=cost(2 * n_src * n_dest * cap * tok * width, n_src * tok * width * 6),
        name="compact",
    )(*xs, *map(in_hbm, after))


def picked_kernel(ids_ref, tok_ref, w_ref, out_ref, ids, toks, weights, sem):
    copies = [
        pltpu.make_async_copy(w_ref, weights, sem.at[0]),
        pltpu.make_async_copy(tok_ref, toks, sem.at[1]),
        pltpu.make_async_copy(ids_ref, ids, sem.at[2]),
    ]
    for copy in copies:
        copy.start()
    for copy in copies:
        copy.wait()
    logits = lax.dot_general(
        weights[...], toks[...], (((0,), (1,)), ((), ())), preferred_element_type=f32
    )
    experts = lax.broadcasted_iota(i32, logits.shape, 0)
    rows = []
    for k in range(ids.shape[0]):
        hit = experts == ids[k : k + 1, :]
        rows.append(jnp.sum(jnp.where(hit, logits, 0.0), axis=0, keepdims=True))
    picked = jnp.concatenate(rows, axis=0)
    for w in range(out_ref.shape[0]):
        out_ref[w] = picked


def front(ids, tokens_in, router_weight, n_width):
    (top, tok), width, experts = ids.shape, tokens_in.shape[1], router_weight.shape[1]
    return pl.pallas_call(
        picked_kernel,
        out_shape=jax.ShapeDtypeStruct((n_width, top, tok), f32),
        in_specs=[HBM] * 3,
        out_specs=VMEM,
        scratch_shapes=[
            pltpu.VMEM((top, tok), i32),
            pltpu.VMEM((tok, width), bf16),
            pltpu.VMEM((width, experts), bf16),
            pltpu.SemaphoreType.DMA((3,)),
        ],
        compiler_params=params(6),
        cost_estimate=cost(2 * tok * width * experts, 2 * tok * width),
        name="picked",
    )(in_hbm(ids), in_hbm(tokens_in), in_hbm(router_weight))


def gates_of(parts):
    logits = jnp.sum(parts, axis=0)
    picked = 1.0 / (1.0 + jnp.exp(-logits))
    totals = jnp.sum(picked, axis=0, keepdims=True)
    return picked, totals


def gate_kernel(per_device, parts_ref, ids_ref, slots_ref, out_ref):
    picked, totals = gates_of(parts_ref[...])
    gates = (route_scale * picked / totals).astype(bf16).astype(f32)
    top, tok = ids_ref.shape
    n_expert, cap = out_ref.shape
    dev, slots = ids_ref[...] // per_device, slots_ref[...]
    dev_rows = lax.broadcasted_iota(i32, (n_expert, tok), 0)
    slot_rows = lax.broadcasted_iota(i32, (cap, tok), 0)
    total = jnp.zeros((n_expert, cap), f32)
    for k in range(top):
        left = jnp.where(dev_rows == dev[k : k + 1], gates[k : k + 1], 0.0).astype(bf16)
        right = jnp.where(slot_rows == slots[k : k + 1], 1.0, 0.0).astype(bf16)
        total = total + lax.dot_general(left, right, (((1,), (1,)), ((), ())), preferred_element_type=f32)
    out_ref[...] = total


def row_dots(chunk, other):
    total = None
    for at in range(0, chunk.shape[1], 128):
        term = chunk[:, at : at + 128].astype(f32) * other[:, at : at + 128].astype(f32)
        total = term if total is None else total + term
    return jnp.sum(total.T, axis=0, keepdims=True)


def fetch(eo_ref, stage, sem, cells, cap):
    copies = []
    for at, src in enumerate(cells):
        rows = eo_ref.at[pl.ds(pl.multiple_of(src * cap, cap), cap), :]
        copies.append(pltpu.make_async_copy(rows, stage.at[at], sem.at[at]))
        copies[-1].start()
    return copies


def fetch_chunks(chunk_refs, stage, sem, cap, first=0):
    copies, at = [], first
    for chunk_ref in chunk_refs:
        for j in range(chunk_ref.shape[0] // cap):
            copies.append(pltpu.make_async_copy(chunk_ref.at[pl.ds(j * cap, cap), :], stage.at[at], sem.at[at]))
            copies[-1].start()
            at += 1
    return copies


def cells_of(batch, side, place):
    return [cell(place, -s, -d) for d in range(side) for s in batch]


def dots_kernel(batch, side, cap, next_batch, eo_ref, *refs):
    chunk_refs = refs[:side]
    out_refs, (held, stage, sem, next_sem) = refs[side:-4], refs[-4:]
    place = here()
    rows = fetch_chunks(chunk_refs, held, sem.at[0], cap)
    others = fetch(eo_ref, stage, sem.at[1], cells_of(batch, side, place), cap)
    ahead = fetch(eo_ref, out_refs[1], next_sem, cells_of(next_batch, side, place), cap) if next_batch else []
    for at in range(len(rows)):
        rows[at].wait()
        others[at].wait()
        out_refs[0][at : at + 1, :] = row_dots(held.at[at], stage.at[at])
    for copy in ahead:
        copy.wait()


def row_dots_call(batch, next_batch, eo, chunks, cap):
    n, width, side = len(batch) * len(chunks), chunks[0].shape[1], len(chunks)
    n_next = len(next_batch) * side
    outs = [jax.ShapeDtypeStruct((n, cap), f32)]
    if n_next:
        outs.append(pltpu.VMEM((n_next, cap, width), bf16))
    return pl.pallas_call(
        functools.partial(dots_kernel, batch, side, cap, next_batch),
        out_shape=outs,
        in_specs=[HBM] * (1 + side),
        out_specs=[VMEM] * len(outs),
        scratch_shapes=[
            pltpu.VMEM((n, cap, width), bf16),
            pltpu.VMEM((n, cap, width), bf16),
            pltpu.SemaphoreType.DMA((2, n)),
            pltpu.SemaphoreType.DMA((max(n_next, 1),)),
        ],
        compiler_params=params(12),
        cost_estimate=cost(2 * n * cap * width, 4 * n * cap * width),
        name="dots",
    )(in_hbm(eo), *map(in_hbm, chunks))


def last_dots_kernel(n_width, batches, side, gate_ref, eo_ref, *refs):
    chunk_refs, early_refs, out_ref = refs[:side], refs[side:-1], refs[-1]
    n_expert = gate_ref.shape[0]
    place = here()
    for e in range(n_expert):
        for w in range(n_width):
            out_ref[2 * (e * n_width + w) + 1] = gate_ref[e : e + 1, :]

    def put(src, row):
        base = src * (2 * n_width)
        for w in range(n_width):
            out_ref[base + 2 * w] = row

    for batch, early in zip(batches[:-1], early_refs):
        for at, src in enumerate(cells_of(batch, side, place)):
            put(src, early[at : at + 1, :])
    for at, src in enumerate(cells_of(batches[-1], side, place)):
        put(src, row_dots(chunk_refs[at], eo_ref.at[at]))


def tail_kernel(n_expert, n_width, per_device, got_ref, parts_ref, ids_ref, slots_ref, tok_ref, lg_ref, router_ref):
    top, tok = ids_ref.shape
    rows = []
    for e in range(n_expert):
        row = got_ref[2 * e * n_width]
        for w in range(1, n_width):
            row = row + got_ref[2 * (e * n_width + w)]
        rows.append(row)
    dots = jnp.concatenate(rows, axis=0)
    cap = dots.shape[1]
    high = dots.astype(bf16)
    low = (dots - high.astype(f32)).astype(bf16)
    both = jnp.concatenate([high, low], axis=0)
    ids, slots = ids_ref[...], slots_ref[...]
    dev = ids // per_device
    slot_rows = lax.broadcasted_iota(i32, (cap, tok), 0)
    dev_rows = lax.broadcasted_iota(i32, (n_expert, tok), 0)
    out = []
    for k in range(top):
        table = jnp.where(slot_rows == slots[k : k + 1], 1.0, 0.0).astype(bf16)
        found = jnp.dot(both, table, preferred_element_type=f32)
        found = found[:n_expert] + found[n_expert:]
        out.append(jnp.sum(jnp.where(dev_rows == dev[k : k + 1], found, 0.0), axis=0, keepdims=True))
    gate_grads = jnp.concatenate(out, axis=0)
    picked, totals = gates_of(parts_ref[...])
    weighted = jnp.sum(gate_grads * picked, axis=0, keepdims=True) / totals
    local = route_scale / totals * (gate_grads - weighted) * picked * (1.0 - picked)
    experts = lax.broadcasted_iota(i32, (lg_ref.shape[0], tok), 0)
    grads = jnp.zeros(lg_ref.shape, f32)
    for k in range(top):
        grads = grads + jnp.where(experts == ids[k : k + 1], local[k : k + 1], 0.0)
    grads = grads.astype(bf16)
    lg_ref[...] = grads
    router_ref[...] = jnp.dot(grads, tok_ref[...], preferred_element_type=f32).astype(bf16)


def scale_kernel(n_width, batches, cap, side, got_ref, lg_ref, w_ref, *refs):
    chunk_refs, (out_ref, input_ref, held, stage, in_sem, sem) = refs[:-6], refs[-6:]
    place = here()
    rows = fetch_chunks(chunk_refs, held, in_sem, cap)
    copies = []
    cells = sum([cells_of(batch, side, place) for batch in batches], [])
    for at, src in enumerate(cells):
        gate = jnp.broadcast_to(got_ref[src * (2 * n_width) + 1], (128, cap)).T
        rows[at].wait()
        for lane in range(0, held.shape[2], 128):
            part = held[at, :, lane : lane + 128].astype(f32)
            stage[at, :, lane : lane + 128] = (part * gate).astype(bf16)
        to = out_ref.at[pl.ds(pl.multiple_of(src * cap, cap), cap), :]
        copies.append(pltpu.make_async_copy(stage.at[at], to, sem.at[at]))
        copies[-1].start()
    input_ref[...] = lax.dot_general(
        lg_ref[...], w_ref[...], (((0,), (1,)), ((), ())), preferred_element_type=f32
    ).astype(bf16)
    for copy in copies:
        copy.wait()


def body(tokens_in, out_grad, router_weight, expert_out, expert_ids, slot_ids):
    n_expert, n_width = lax.axis_size("expert"), lax.axis_size("width")
    side = int(round(n_expert**0.5))
    tok, width = out_grad.shape
    top = expert_ids.shape[1]
    experts = router_weight.shape[1]
    per_device = experts // n_expert
    cap = tok * top // n_expert

    def send(x, shift, second):
        return lax.ppermute(x, AXES, line_shift(n_expert, n_width, shift, second))

    ids, slots = expert_ids.T, slot_ids.T
    half = tok // 2
    first, last = pl.pallas_call(
        functools.partial(pack_kernel, per_device),
        out_shape=[
            jax.ShapeDtypeStruct((half, width), bf16),
            jax.ShapeDtypeStruct((tok - half + top, width), bf16),
        ],
        in_specs=[HBM] * 3,
        out_specs=[VMEM] * 2,
        scratch_shapes=[
            pltpu.VMEM((top, tok), i32),
            pltpu.VMEM((top, tok), i32),
            pltpu.SemaphoreType.DMA((4,)),
        ],
        compiler_params=params(4),
        cost_estimate=cost(0, 4 * tok * width),
        name="pack",
    )(in_hbm(out_grad), in_hbm(ids), in_hbm(slots))
    up_first = send(first, 1, False)
    down_last = send(last, side - 1, False)
    up_last = send(last, 1, False)
    down_first = send(first, side - 1, False)
    far = [send(up_first, 1, False), send(down_last, side - 1, False)]
    sources = {0: [first, last], 1: [up_first, up_last], side - 1: [down_first, down_last], 2: far}
    batches = [[0, 1, side - 1], [2]]

    sent_parts = front(ids, tokens_in, router_weight, n_width)
    parts = lax.all_to_all(sent_parts, "width", 0, 0, tiled=True)

    landed, after = [], []
    for batch in batches:
        chunks = compact([sources[s] for s in batch], after, tok, cap, side)
        after = [chunks[0]]
        group = [chunks[0]]
        for d in range(1, side):
            group.append(send(chunks[d], d, True))
        landed.append(group)

    gates = pl.pallas_call(
        functools.partial(gate_kernel, per_device),
        out_shape=jax.ShapeDtypeStruct((n_expert, cap), f32),
        in_specs=[VMEM] * 3,
        out_specs=VMEM,
        compiler_params=params(4),
        cost_estimate=cost(2 * top * n_expert * cap * tok, 4 * n_width * top * tok),
        name="gates",
    )(parts, ids, slots)

    early = []
    for b, batch in enumerate(batches[:-1]):
        next_batch = batches[-1] if b == len(batches) - 2 else []
        outs = row_dots_call(batch, next_batch, expert_out, landed[b], cap)
        early.append(outs[0])
    sent = pl.pallas_call(
        functools.partial(last_dots_kernel, n_width, batches, side),
        out_shape=jax.ShapeDtypeStruct((2 * n_expert * n_width, 1, cap), f32),
        in_specs=[VMEM] * (2 + side + len(early)),
        out_specs=VMEM,
        compiler_params=params(6),
        cost_estimate=cost(2 * side * cap * width, 4 * side * cap * width),
        name="last_dots",
    )(gates, outs[1], *landed[-1], *early)
    got = lax.all_to_all(sent, AXES, 0, 0, tiled=True)

    logit_grads, router_part = pl.pallas_call(
        functools.partial(tail_kernel, n_expert, n_width, per_device),
        out_shape=[
            jax.ShapeDtypeStruct((experts, tok), bf16),
            jax.ShapeDtypeStruct((experts, width), bf16),
        ],
        in_specs=[VMEM] * 5,
        out_specs=[VMEM] * 2,
        compiler_params=params(8),
        cost_estimate=cost(2 * tok * width * experts, 2 * tok * width),
        name="tail",
    )(got, parts, ids, slots, tokens_in)
    blocks = lax.all_to_all(router_part.reshape(n_expert, per_device, width), "expert", 0, 0, tiled=True)
    flat = sum(landed, [])
    expert_grad, input_grad = pl.pallas_call(
        functools.partial(scale_kernel, n_width, batches, cap, side),
        out_shape=[
            jax.ShapeDtypeStruct(expert_out.shape, bf16),
            jax.ShapeDtypeStruct((tok, width), bf16),
        ],
        in_specs=[VMEM] * 3 + [HBM] * len(flat),
        out_specs=[HBM, VMEM],
        scratch_shapes=[
            pltpu.VMEM((n_expert, cap, width), bf16),
            pltpu.VMEM((n_expert, cap, width), bf16),
            pltpu.SemaphoreType.DMA((n_expert,)),
            pltpu.SemaphoreType.DMA((n_expert,)),
        ],
        compiler_params=params(16),
        cost_estimate=cost(2 * tok * width * experts, 4 * n_expert * cap * width),
        name="scale",
    )(got, logit_grads, router_weight, *map(in_hbm, flat))
    router_grad = jnp.sum(blocks.astype(f32), axis=0).T
    return (expert_grad, router_grad, input_grad)


def solution(mesh):
    return jax.shard_map(
        body,
        mesh=mesh,
        in_specs=(
            P("expert", "width"),
            P("expert", "width"),
            P("width", None),
            P("expert", "width"),
            P("expert", None),
            P("expert", None),
        ),
        out_specs=(P("expert", "width"), P("width", "expert"), P("expert", "width")),
        check_vma=False,
    )
```

```python
import functools

import jax
import jax.numpy as jnp
from jax import lax
from jax.experimental import pallas as pl
from jax.experimental.pallas import tpu as pltpu
from jax.sharding import PartitionSpec as P


route_scale = 2.5
AXES = ("expert", "width")
f32, bf16, i32 = jnp.float32, jnp.bfloat16, jnp.int32
PARTS = (((2,), (1, 3), (0,)), ((2, 1, 3, 0),))
DOTS = ((0,), (2,), (1, 3))
VMEM = pl.BlockSpec(memory_space=pltpu.VMEM)
SMEM = pl.BlockSpec(memory_space=pltpu.SMEM)
ANY = pl.BlockSpec(memory_space=pl.ANY)
HBM = pl.BlockSpec(memory_space=pltpu.HBM)


def params(mib):
    return pltpu.CompilerParams(vmem_limit_bytes=mib * 1024 * 1024)


def cost(flops, moved):
    return pl.CostEstimate(flops=flops, bytes_accessed=moved, transcendentals=0)


def line_shift(n_expert, n_width, shift, second):
    side = int(round(n_expert**0.5))
    pairs = []
    for e in range(n_expert):
        y, z = e // side, e % side
        for w in range(n_width):
            if (w % 2 == 0) != second:
                to = ((y + shift) % side) * side + z
            else:
                to = y * side + (z + shift) % side
            pairs.append((e * n_width + w, to * n_width + w))
    return pairs


def here():
    n_expert = lax.axis_size("expert")
    side = int(round(n_expert**0.5))
    me = lax.axis_index("expert")
    return side, lax.div(me, side), lax.rem(me, side), lax.rem(lax.axis_index("width"), 2)


def cell(place, along, across):
    side, y, z, core = place
    along, across = along % side, across % side
    first = lax.rem(y + along, side) * side + lax.rem(z + across, side)
    second = lax.rem(y + across, side) * side + lax.rem(z + along, side)
    return jnp.where(core == 0, first, second)


def in_hbm(x):
    return pltpu.with_memory_space_constraint(x, pltpu.HBM)


def pack_kernel(per_device, x_ref, ids_ref, slots_ref, first_ref, last_ref, held_ids, held_slots, sem):
    tok, width = x_ref.shape
    top, half = ids_ref.shape[0], first_ref.shape[0]
    copies = [
        pltpu.make_async_copy(ids_ref, held_ids, sem.at[0]),
        pltpu.make_async_copy(slots_ref, held_slots, sem.at[1]),
        pltpu.make_async_copy(x_ref.at[pl.ds(0, half), :], first_ref, sem.at[2]),
        pltpu.make_async_copy(x_ref.at[pl.ds(half, tok - half), :], last_ref.at[pl.ds(0, tok - half), :], sem.at[3]),
    ]
    for copy in copies:
        copy.start()
    copies[0].wait()
    copies[1].wait()
    dev = (held_ids[...] // per_device).astype(f32)
    slots = held_slots[...].astype(f32)
    rest = jnp.zeros((top, width - 2 * tok), f32)
    last_ref[tok - half :, :] = jnp.concatenate([dev, slots, rest], axis=1).astype(bf16)
    copies[2].wait()
    copies[3].wait()


def compact_kernel(parts, tok, cap, dests, halves, *refs):
    n_in, n_half, n_dest = sum(parts), len(halves), len(dests)
    x_refs, (stage, sem) = refs[:n_in], refs[-2:]
    out_refs, half_refs = refs[-2 - n_half - n_dest : -2 - n_half], refs[-2 - n_half : -2]
    place = here()
    copies = []
    for at, (j, rows, first) in enumerate(halves):
        part = x_refs[j].at[pl.ds(first, rows), :]
        copies.append(pltpu.make_async_copy(part, half_refs[at], sem.at[n_dest + at]))
        copies[-1].start()
    for out, d in enumerate(dests):
        at = 0
        for j, count in enumerate(parts):
            mine_refs = x_refs[at : at + count]
            at += count
            last = mine_refs[-1].shape[0]
            top = sum(ref.shape[0] for ref in mine_refs) - tok
            info = mine_refs[-1][last - top :, :].astype(f32)
            dev, slots = info[:, :tok], info[:, tok : 2 * tok]
            mine = dev == cell(place, 0, d).astype(f32)
            slot = jnp.sum(jnp.where(mine, slots + 1.0, 0.0), axis=0, keepdims=True).astype(i32) - 1
            got, first = None, 0
            for ref in mine_refs:
                rows = min(ref.shape[0], tok - first)
                want = lax.broadcasted_iota(i32, (cap, rows), 0)
                table = jnp.where(want == slot[:, first : first + rows], 1.0, 0.0).astype(bf16)
                term = jnp.dot(table, ref[:rows, :], preferred_element_type=f32)
                got = term if got is None else got + term
                first += rows
            stage[out, j * cap : (j + 1) * cap, :] = got.astype(bf16)
        copies.append(pltpu.make_async_copy(stage.at[out], out_refs[out], sem.at[out]))
        copies[-1].start()
    for copy in copies:
        copy.wait()


def compact(sources, after, tok, cap, dests, halves=()):
    n_src, width, n_dest = len(sources), sources[0][0].shape[1], len(dests)
    xs = sum(sources, [])
    outs = [pltpu.HBM((n_src * cap, width), bf16)] * n_dest
    outs += [pltpu.HBM((rows, width), bf16) for _, rows, _ in halves]
    return pl.pallas_call(
        functools.partial(compact_kernel, [len(x) for x in sources], tok, cap, dests, halves),
        out_shape=outs,
        in_specs=[VMEM] * len(xs) + [HBM] * len(after),
        out_specs=[HBM] * len(outs),
        scratch_shapes=[
            pltpu.VMEM((n_dest, n_src * cap, width), bf16),
            pltpu.SemaphoreType.DMA((n_dest + len(halves),)),
        ],
        compiler_params=params(12),
        cost_estimate=cost(2 * n_src * n_dest * cap * tok * width, n_src * tok * width * 6),
        name="compact",
    )(*xs, *map(in_hbm, after))


def picked_kernel(ids_ref, tok_ref, w_ref, out_ref, ids, toks, weights, sem):
    copies = [
        pltpu.make_async_copy(w_ref, weights, sem.at[0]),
        pltpu.make_async_copy(tok_ref, toks, sem.at[1]),
        pltpu.make_async_copy(ids_ref, ids, sem.at[2]),
    ]
    for copy in copies:
        copy.start()
    for copy in copies:
        copy.wait()
    logits = lax.dot_general(
        weights[...], toks[...], (((0,), (1,)), ((), ())), preferred_element_type=f32
    )
    experts = lax.broadcasted_iota(i32, logits.shape, 0)
    rows = []
    for k in range(ids.shape[0]):
        hit = experts == ids[k : k + 1, :]
        rows.append(jnp.sum(jnp.where(hit, logits, 0.0), axis=0, keepdims=True))
    picked = jnp.concatenate(rows, axis=0)
    for w in range(out_ref.shape[0]):
        out_ref[w] = picked


def front(ids, tokens_in, router_weight, n_width):
    (top, tok), width, experts = ids.shape, tokens_in.shape[1], router_weight.shape[1]
    return pl.pallas_call(
        picked_kernel,
        out_shape=jax.ShapeDtypeStruct((n_width, top, tok), f32),
        in_specs=[HBM] * 3,
        out_specs=VMEM,
        scratch_shapes=[
            pltpu.VMEM((top, tok), i32),
            pltpu.VMEM((tok, width), bf16),
            pltpu.VMEM((width, experts), bf16),
            pltpu.SemaphoreType.DMA((3,)),
        ],
        compiler_params=params(6),
        cost_estimate=cost(2 * tok * width * experts, 2 * tok * width),
        name="picked",
    )(in_hbm(ids), in_hbm(tokens_in), in_hbm(router_weight))


def gates_of(parts):
    logits = jnp.sum(parts, axis=0)
    picked = 1.0 / (1.0 + jnp.exp(-logits))
    totals = jnp.sum(picked, axis=0, keepdims=True)
    return picked, totals


def gate_kernel(per_device, parts_ref, ids_ref, slots_ref, out_ref):
    picked, totals = gates_of(parts_ref[...])
    gates = (route_scale * picked / totals).astype(bf16).astype(f32)
    top, tok = ids_ref.shape
    n_expert, cap = out_ref.shape
    dev, slots = ids_ref[...] // per_device, slots_ref[...]
    dev_rows = lax.broadcasted_iota(i32, (n_expert, tok), 0)
    slot_rows = lax.broadcasted_iota(i32, (cap, tok), 0)
    total = jnp.zeros((n_expert, cap), f32)
    for k in range(top):
        left = jnp.where(dev_rows == dev[k : k + 1], gates[k : k + 1], 0.0).astype(bf16)
        right = jnp.where(slot_rows == slots[k : k + 1], 1.0, 0.0).astype(bf16)
        total = total + lax.dot_general(left, right, (((1,), (1,)), ((), ())), preferred_element_type=f32)
    out_ref[...] = total


def row_dots(chunk, other):
    total = None
    for at in range(0, chunk.shape[1], 128):
        term = chunk[:, at : at + 128].astype(f32) * other[:, at : at + 128].astype(f32)
        total = term if total is None else total + term
    return jnp.sum(total.T, axis=0, keepdims=True)


def fetch(eo_ref, stage, sem, cells, cap):
    copies = []
    for at, src in enumerate(cells):
        rows = eo_ref.at[pl.ds(pl.multiple_of(src * cap, cap), cap), :]
        copies.append(pltpu.make_async_copy(rows, stage.at[at], sem.at[at]))
        copies[-1].start()
    return copies


def fetch_chunks(chunk_refs, stage, sem, cap, first=0):
    copies, at = [], first
    for chunk_ref in chunk_refs:
        for j in range(chunk_ref.shape[0] // cap):
            copies.append(pltpu.make_async_copy(chunk_ref.at[pl.ds(j * cap, cap), :], stage.at[at], sem.at[at]))
            copies[-1].start()
            at += 1
    return copies


def cells_of(batch, dests, place):
    return [cell(place, -s, -d) for d in dests for s in batch]


def dots_kernel(batch, dests, cap, ahead_cells, eo_ref, *refs):
    chunk_refs = refs[: len(dests)]
    out_refs, (held, stage, sem, next_sem) = refs[len(dests) : -4], refs[-4:]
    place = here()
    rows = fetch_chunks(chunk_refs, held, sem.at[0], cap)
    others = fetch(eo_ref, stage, sem.at[1], cells_of(batch, dests, place), cap)
    ahead = fetch(eo_ref, out_refs[1], next_sem, cells_of(*ahead_cells, place), cap) if ahead_cells else []
    for at in range(len(rows)):
        rows[at].wait()
        others[at].wait()
        out_refs[0][at : at + 1, :] = row_dots(held.at[at], stage.at[at])
    for copy in ahead:
        copy.wait()


def row_dots_call(batch, dests, ahead_cells, eo, chunks, cap):
    n, width = len(batch) * len(dests), chunks[0].shape[1]
    n_next = len(ahead_cells[0]) * len(ahead_cells[1]) if ahead_cells else 0
    outs = [jax.ShapeDtypeStruct((n, cap), f32)]
    if n_next:
        outs.append(pltpu.VMEM((n_next, cap, width), bf16))
    return pl.pallas_call(
        functools.partial(dots_kernel, batch, dests, cap, ahead_cells),
        out_shape=outs,
        in_specs=[HBM] * (1 + len(dests)),
        out_specs=[VMEM] * len(outs),
        scratch_shapes=[
            pltpu.VMEM((n, cap, width), bf16),
            pltpu.VMEM((n, cap, width), bf16),
            pltpu.SemaphoreType.DMA((2, n)),
            pltpu.SemaphoreType.DMA((max(n_next, 1),)),
        ],
        compiler_params=params(8),
        cost_estimate=cost(2 * n * cap * width, 4 * n * cap * width),
        name="dots",
    )(in_hbm(eo), *map(in_hbm, chunks))


def last_dots_kernel(n_width, groups, last, side, gate_ref, eo_ref, *refs):
    chunk_refs, early_refs, out_ref = refs[:side], refs[side:-1], refs[-1]
    n_expert = gate_ref.shape[0]
    place = here()
    for e in range(n_expert):
        for w in range(n_width):
            out_ref[2 * (e * n_width + w) + 1] = gate_ref[e : e + 1, :]

    def put(src, row):
        base = src * (2 * n_width)
        for w in range(n_width):
            out_ref[base + 2 * w] = row

    for (batch, dests), early in zip(groups, early_refs):
        for at, src in enumerate(cells_of(batch, dests, place)):
            put(src, early[at : at + 1, :])
    for at, src in enumerate(cells_of(last, range(side), place)):
        put(src, row_dots(chunk_refs[at], eo_ref.at[at]))


def tail_kernel(n_expert, n_width, per_device, got_ref, parts_ref, ids_ref, slots_ref, tok_ref, lg_ref, router_ref):
    top, tok = ids_ref.shape
    rows = []
    for e in range(n_expert):
        row = got_ref[2 * e * n_width]
        for w in range(1, n_width):
            row = row + got_ref[2 * (e * n_width + w)]
        rows.append(row)
    dots = jnp.concatenate(rows, axis=0)
    cap = dots.shape[1]
    high = dots.astype(bf16)
    low = (dots - high.astype(f32)).astype(bf16)
    both = jnp.concatenate([high, low], axis=0)
    ids, slots = ids_ref[...], slots_ref[...]
    dev = ids // per_device
    slot_rows = lax.broadcasted_iota(i32, (cap, tok), 0)
    dev_rows = lax.broadcasted_iota(i32, (n_expert, tok), 0)
    out = []
    for k in range(top):
        table = jnp.where(slot_rows == slots[k : k + 1], 1.0, 0.0).astype(bf16)
        found = jnp.dot(both, table, preferred_element_type=f32)
        found = found[:n_expert] + found[n_expert:]
        out.append(jnp.sum(jnp.where(dev_rows == dev[k : k + 1], found, 0.0), axis=0, keepdims=True))
    gate_grads = jnp.concatenate(out, axis=0)
    picked, totals = gates_of(parts_ref[...])
    weighted = jnp.sum(gate_grads * picked, axis=0, keepdims=True) / totals
    local = route_scale / totals * (gate_grads - weighted) * picked * (1.0 - picked)
    experts = lax.broadcasted_iota(i32, (lg_ref.shape[0], tok), 0)
    grads = jnp.zeros(lg_ref.shape, f32)
    for k in range(top):
        grads = grads + jnp.where(experts == ids[k : k + 1], local[k : k + 1], 0.0)
    grads = grads.astype(bf16)
    lg_ref[...] = grads
    router_ref[...] = jnp.dot(grads, tok_ref[...], preferred_element_type=f32).astype(bf16)


def scale_kernel(n_width, batches, cap, side, got_ref, lg_ref, w_ref, *refs):
    chunk_refs, (out_ref, input_ref, held, stage, in_sem, sem) = refs[:-6], refs[-6:]
    place = here()
    rows = fetch_chunks(chunk_refs, held, in_sem, cap)
    copies = []
    cells = sum([cells_of(batch, range(side), place) for batch in batches], [])
    for at, src in enumerate(cells):
        gate = jnp.broadcast_to(got_ref[src * (2 * n_width) + 1], (128, cap)).T
        rows[at].wait()
        for lane in range(0, held.shape[2], 128):
            part = held[at, :, lane : lane + 128].astype(f32)
            stage[at, :, lane : lane + 128] = (part * gate).astype(bf16)
        to = out_ref.at[pl.ds(pl.multiple_of(src * cap, cap), cap), :]
        copies.append(pltpu.make_async_copy(stage.at[at], to, sem.at[at]))
        copies[-1].start()
    input_ref[...] = lax.dot_general(
        lg_ref[...], w_ref[...], (((0,), (1,)), ((), ())), preferred_element_type=f32
    ).astype(bf16)
    for copy in copies:
        copy.wait()


def body(tokens_in, out_grad, router_weight, expert_out, expert_ids, slot_ids):
    n_expert, n_width = lax.axis_size("expert"), lax.axis_size("width")
    side = int(round(n_expert**0.5))
    tok, width = out_grad.shape
    top = expert_ids.shape[1]
    experts = router_weight.shape[1]
    per_device = experts // n_expert
    cap = tok * top // n_expert

    def send(x, shift, second):
        return lax.ppermute(x, AXES, line_shift(n_expert, n_width, shift, second))

    ids, slots = expert_ids.T, slot_ids.T
    half = tok // 2
    first, last = pl.pallas_call(
        functools.partial(pack_kernel, per_device),
        out_shape=[
            jax.ShapeDtypeStruct((half, width), bf16),
            jax.ShapeDtypeStruct((tok - half + top, width), bf16),
        ],
        in_specs=[HBM] * 3,
        out_specs=[VMEM] * 2,
        scratch_shapes=[
            pltpu.VMEM((top, tok), i32),
            pltpu.VMEM((top, tok), i32),
            pltpu.SemaphoreType.DMA((4,)),
        ],
        compiler_params=params(4),
        cost_estimate=cost(0, 4 * tok * width),
        name="pack",
    )(in_hbm(out_grad), in_hbm(ids), in_hbm(slots))
    up_first = send(first, 1, False)
    down_last = send(last, side - 1, False)
    up_last = send(last, 1, False)
    down_first = send(first, side - 1, False)
    far = [send(up_first, 1, False), send(down_last, side - 1, False)]
    sources = {0: [first, last], 1: [up_first, up_last], side - 1: [down_first, down_last], 2: far}
    batches = [[0, 1, side - 1], [2]]

    sent_parts = front(ids, tokens_in, router_weight, n_width)
    parts = lax.all_to_all(sent_parts, "width", 0, 0, tiled=True)

    landed, after = [], []
    for b, batch in enumerate(batches):
        group = [None] * side
        for dests in PARTS[b]:
            chunks = compact([sources[s] for s in batch], after, tok, cap, dests)
            after = [chunks[0]]
            for d, chunk in zip(dests, chunks):
                group[d] = chunk if d == 0 else send(chunk, d, True)
        landed.append(group)

    gates = pl.pallas_call(
        functools.partial(gate_kernel, per_device),
        out_shape=jax.ShapeDtypeStruct((n_expert, cap), f32),
        in_specs=[VMEM] * 3,
        out_specs=VMEM,
        compiler_params=params(4),
        cost_estimate=cost(2 * top * n_expert * cap * tok, 4 * n_width * top * tok),
        name="gates",
    )(parts, ids, slots)

    early, groups, ahead = [], [], None
    for b, batch in enumerate(batches[:-1]):
        for dests in DOTS:
            ahead_cells = (batches[-1], range(side)) if ahead is None else ()
            outs = row_dots_call(batch, dests, ahead_cells, expert_out, [landed[b][d] for d in dests], cap)
            ahead = outs[1] if ahead is None else ahead
            early.append(outs[0])
            groups.append((batch, dests))
    sent = pl.pallas_call(
        functools.partial(last_dots_kernel, n_width, groups, batches[-1], side),
        out_shape=jax.ShapeDtypeStruct((2 * n_expert * n_width, 1, cap), f32),
        in_specs=[VMEM] * (2 + side + len(early)),
        out_specs=VMEM,
        compiler_params=params(6),
        cost_estimate=cost(2 * side * cap * width, 4 * side * cap * width),
        name="last_dots",
    )(gates, ahead, *landed[-1], *early)
    got = lax.all_to_all(sent, AXES, 0, 0, tiled=True)

    logit_grads, router_part = pl.pallas_call(
        functools.partial(tail_kernel, n_expert, n_width, per_device),
        out_shape=[
            jax.ShapeDtypeStruct((experts, tok), bf16),
            jax.ShapeDtypeStruct((experts, width), bf16),
        ],
        in_specs=[VMEM] * 5,
        out_specs=[VMEM] * 2,
        compiler_params=params(8),
        cost_estimate=cost(2 * tok * width * experts, 2 * tok * width),
        name="tail",
    )(got, parts, ids, slots, tokens_in)
    blocks = lax.all_to_all(router_part.reshape(n_expert, per_device, width), "expert", 0, 0, tiled=True)
    flat = sum(landed, [])
    expert_grad, input_grad = pl.pallas_call(
        functools.partial(scale_kernel, n_width, batches, cap, side),
        out_shape=[
            jax.ShapeDtypeStruct(expert_out.shape, bf16),
            jax.ShapeDtypeStruct((tok, width), bf16),
        ],
        in_specs=[VMEM] * 3 + [HBM] * len(flat),
        out_specs=[HBM, VMEM],
        scratch_shapes=[
            pltpu.VMEM((n_expert, cap, width), bf16),
            pltpu.VMEM((n_expert, cap, width), bf16),
            pltpu.SemaphoreType.DMA((n_expert,)),
            pltpu.SemaphoreType.DMA((n_expert,)),
        ],
        compiler_params=params(16),
        cost_estimate=cost(2 * tok * width * experts, 4 * n_expert * cap * width),
        name="scale",
    )(got, logit_grads, router_weight, *map(in_hbm, flat))
    router_grad = jnp.sum(blocks.astype(f32), axis=0).T
    return (expert_grad, router_grad, input_grad)


def solution(mesh):
    return jax.shard_map(
        body,
        mesh=mesh,
        in_specs=(
            P("expert", "width"),
            P("expert", "width"),
            P("width", None),
            P("expert", "width"),
            P("expert", None),
            P("expert", None),
        ),
        out_specs=(P("expert", "width"), P("width", "expert"), P("expert", "width")),
        check_vma=False,
    )
```

```python
import functools

import jax
import jax.numpy as jnp
from jax import lax
from jax.experimental import pallas as pl
from jax.experimental.pallas import tpu as pltpu
from jax.sharding import PartitionSpec as P


route_scale = 2.5
AXES = ("expert", "width")
f32, bf16, i32 = jnp.float32, jnp.bfloat16, jnp.int32
DIRECT = False
PARTS = (((2,), (1,), (3,), (0,)), ((2,), (1, 3, 0)))
DOTS = ((0,), (2,), (1, 3))
VMEM = pl.BlockSpec(memory_space=pltpu.VMEM)
SMEM = pl.BlockSpec(memory_space=pltpu.SMEM)
ANY = pl.BlockSpec(memory_space=pl.ANY)
HBM = pl.BlockSpec(memory_space=pltpu.HBM)


def params(mib):
    return pltpu.CompilerParams(vmem_limit_bytes=mib * 1024 * 1024)


def cost(flops, moved):
    return pl.CostEstimate(flops=flops, bytes_accessed=moved, transcendentals=0)


def line_shift(n_expert, n_width, shift, second):
    side = int(round(n_expert**0.5))
    pairs = []
    for e in range(n_expert):
        y, z = e // side, e % side
        for w in range(n_width):
            if (w % 2 == 0) != second:
                to = ((y + shift) % side) * side + z
            else:
                to = y * side + (z + shift) % side
            pairs.append((e * n_width + w, to * n_width + w))
    return pairs


def here():
    n_expert = lax.axis_size("expert")
    side = int(round(n_expert**0.5))
    me = lax.axis_index("expert")
    return side, lax.div(me, side), lax.rem(me, side), lax.rem(lax.axis_index("width"), 2)


def cell(place, along, across):
    side, y, z, core = place
    along, across = along % side, across % side
    first = lax.rem(y + along, side) * side + lax.rem(z + across, side)
    second = lax.rem(y + across, side) * side + lax.rem(z + along, side)
    return jnp.where(core == 0, first, second)


def in_hbm(x):
    return pltpu.with_memory_space_constraint(x, pltpu.HBM)


def pack_kernel(per_device, x_ref, ids_ref, slots_ref, first_ref, last_ref, held_ids, held_slots, sem):
    tok, width = x_ref.shape
    top, half = ids_ref.shape[0], first_ref.shape[0]
    copies = [
        pltpu.make_async_copy(ids_ref, held_ids, sem.at[0]),
        pltpu.make_async_copy(slots_ref, held_slots, sem.at[1]),
        pltpu.make_async_copy(x_ref.at[pl.ds(0, half), :], first_ref, sem.at[2]),
        pltpu.make_async_copy(x_ref.at[pl.ds(half, tok - half), :], last_ref.at[pl.ds(0, tok - half), :], sem.at[3]),
    ]
    for copy in copies:
        copy.start()
    copies[0].wait()
    copies[1].wait()
    dev = (held_ids[...] // per_device).astype(f32)
    slots = held_slots[...].astype(f32)
    rest = jnp.zeros((top, width - 2 * tok), f32)
    last_ref[tok - half :, :] = jnp.concatenate([dev, slots, rest], axis=1).astype(bf16)
    copies[2].wait()
    copies[3].wait()


def compact_kernel(parts, tok, cap, dests, direct, *refs):
    n_in, n_dest = sum(parts), len(dests)
    x_refs = refs[:n_in]
    out_refs = refs[n_in : n_in + n_dest]
    place = here()
    copies = []
    for out, d in enumerate(dests):
        at = 0
        for j, count in enumerate(parts):
            mine_refs = x_refs[at : at + count]
            at += count
            last = mine_refs[-1].shape[0]
            top = sum(ref.shape[0] for ref in mine_refs) - tok
            info = mine_refs[-1][last - top :, :].astype(f32)
            dev, slots = info[:, :tok], info[:, tok : 2 * tok]
            mine = dev == cell(place, 0, d).astype(f32)
            slot = jnp.sum(jnp.where(mine, slots + 1.0, 0.0), axis=0, keepdims=True).astype(i32) - 1
            got, first = None, 0
            for ref in mine_refs:
                rows = min(ref.shape[0], tok - first)
                want = lax.broadcasted_iota(i32, (cap, rows), 0)
                table = jnp.where(want == slot[:, first : first + rows], 1.0, 0.0).astype(bf16)
                term = jnp.dot(table, ref[:rows, :], preferred_element_type=f32)
                got = term if got is None else got + term
                first += rows
            if direct:
                out_refs[out][j * cap : (j + 1) * cap, :] = got.astype(bf16)
            else:
                stage, sem = refs[-2:]
                stage[out, j] = got.astype(bf16)
                to = out_refs[out].at[pl.ds(j * cap, cap), :]
                copies.append(pltpu.make_async_copy(stage.at[out, j], to, sem.at[out, j]))
                copies[-1].start()
    for copy in copies:
        copy.wait()


def compact(sources, tok, cap, dests):
    n_src, width, n_dest = len(sources), sources[0][0].shape[1], len(dests)
    xs = sum(sources, [])
    direct = DIRECT and 0 not in dests
    shape = (n_src * cap, width)
    scratch = [pltpu.VMEM((n_dest, n_src, cap, width), bf16), pltpu.SemaphoreType.DMA((n_dest, n_src))]
    return pl.pallas_call(
        functools.partial(compact_kernel, [len(x) for x in sources], tok, cap, dests, direct),
        out_shape=[jax.ShapeDtypeStruct(shape, bf16) if direct else pltpu.HBM(shape, bf16)] * n_dest,
        in_specs=[VMEM] * len(xs),
        out_specs=[VMEM if direct else HBM] * n_dest,
        scratch_shapes=[] if direct else scratch,
        compiler_params=params(8),
        cost_estimate=cost(2 * n_src * n_dest * cap * tok * width, n_src * tok * width * 6),
        name="compact",
    )(*xs)


def picked_kernel(ids_ref, tok_ref, w_ref, out_ref, ids, toks, weights, sem):
    copies = [
        pltpu.make_async_copy(w_ref, weights, sem.at[0]),
        pltpu.make_async_copy(tok_ref, toks, sem.at[1]),
        pltpu.make_async_copy(ids_ref, ids, sem.at[2]),
    ]
    for copy in copies:
        copy.start()
    for copy in copies:
        copy.wait()
    logits = lax.dot_general(
        weights[...], toks[...], (((0,), (1,)), ((), ())), preferred_element_type=f32
    )
    experts = lax.broadcasted_iota(i32, logits.shape, 0)
    rows = []
    for k in range(ids.shape[0]):
        hit = experts == ids[k : k + 1, :]
        rows.append(jnp.sum(jnp.where(hit, logits, 0.0), axis=0, keepdims=True))
    picked = jnp.concatenate(rows, axis=0)
    for w in range(out_ref.shape[0]):
        out_ref[w] = picked


def front(ids, tokens_in, router_weight, n_width):
    (top, tok), width, experts = ids.shape, tokens_in.shape[1], router_weight.shape[1]
    return pl.pallas_call(
        picked_kernel,
        out_shape=jax.ShapeDtypeStruct((n_width, top, tok), f32),
        in_specs=[HBM] * 3,
        out_specs=VMEM,
        scratch_shapes=[
            pltpu.VMEM((top, tok), i32),
            pltpu.VMEM((tok, width), bf16),
            pltpu.VMEM((width, experts), bf16),
            pltpu.SemaphoreType.DMA((3,)),
        ],
        compiler_params=params(6),
        cost_estimate=cost(2 * tok * width * experts, 2 * tok * width),
        name="picked",
    )(in_hbm(ids), in_hbm(tokens_in), in_hbm(router_weight))


def gates_of(parts):
    logits = jnp.sum(parts, axis=0)
    picked = 1.0 / (1.0 + jnp.exp(-logits))
    totals = jnp.sum(picked, axis=0, keepdims=True)
    return picked, totals


def gate_kernel(per_device, parts_ref, ids_ref, slots_ref, out_ref):
    picked, totals = gates_of(parts_ref[...])
    gates = (route_scale * picked / totals).astype(bf16).astype(f32)
    top, tok = ids_ref.shape
    n_expert, cap = out_ref.shape
    dev, slots = ids_ref[...] // per_device, slots_ref[...]
    dev_rows = lax.broadcasted_iota(i32, (n_expert, tok), 0)
    slot_rows = lax.broadcasted_iota(i32, (cap, tok), 0)
    total = jnp.zeros((n_expert, cap), f32)
    for k in range(top):
        left = jnp.where(dev_rows == dev[k : k + 1], gates[k : k + 1], 0.0).astype(bf16)
        right = jnp.where(slot_rows == slots[k : k + 1], 1.0, 0.0).astype(bf16)
        total = total + lax.dot_general(left, right, (((1,), (1,)), ((), ())), preferred_element_type=f32)
    out_ref[...] = total


def row_dots(chunk, other):
    total = None
    for at in range(0, chunk.shape[1], 128):
        term = chunk[:, at : at + 128].astype(f32) * other[:, at : at + 128].astype(f32)
        total = term if total is None else total + term
    return jnp.sum(total.T, axis=0, keepdims=True)


def fetch(eo_ref, stage, sem, cells, cap):
    copies = []
    for at, src in enumerate(cells):
        rows = eo_ref.at[pl.ds(pl.multiple_of(src * cap, cap), cap), :]
        copies.append(pltpu.make_async_copy(rows, stage.at[at], sem.at[at]))
        copies[-1].start()
    return copies


def fetch_chunks(chunk_refs, stage, sem, cap, first=0):
    copies, at = [], first
    for chunk_ref in chunk_refs:
        for j in range(chunk_ref.shape[0] // cap):
            copies.append(pltpu.make_async_copy(chunk_ref.at[pl.ds(j * cap, cap), :], stage.at[at], sem.at[at]))
            copies[-1].start()
            at += 1
    return copies


def cells_of(batch, dests, place):
    return [cell(place, -s, -d) for d in dests for s in batch]


def dots_kernel(batch, dests, cap, ahead_cells, eo_ref, *refs):
    chunk_refs = refs[: len(dests)]
    out_refs, (held, stage, sem, next_sem) = refs[len(dests) : -4], refs[-4:]
    place = here()
    rows = fetch_chunks(chunk_refs, held, sem.at[0], cap)
    others = fetch(eo_ref, stage, sem.at[1], cells_of(batch, dests, place), cap)
    ahead = fetch(eo_ref, out_refs[1], next_sem, cells_of(*ahead_cells, place), cap) if ahead_cells else []
    for at in range(len(rows)):
        rows[at].wait()
        others[at].wait()
        out_refs[0][at : at + 1, :] = row_dots(held.at[at], stage.at[at])
    for copy in ahead:
        copy.wait()


def row_dots_call(batch, dests, ahead_cells, eo, chunks, cap):
    n, width = len(batch) * len(dests), chunks[0].shape[1]
    n_next = len(ahead_cells[0]) * len(ahead_cells[1]) if ahead_cells else 0
    outs = [jax.ShapeDtypeStruct((n, cap), f32)]
    if n_next:
        outs.append(pltpu.VMEM((n_next, cap, width), bf16))
    return pl.pallas_call(
        functools.partial(dots_kernel, batch, dests, cap, ahead_cells),
        out_shape=outs,
        in_specs=[HBM] * (1 + len(dests)),
        out_specs=[VMEM] * len(outs),
        scratch_shapes=[
            pltpu.VMEM((n, cap, width), bf16),
            pltpu.VMEM((n, cap, width), bf16),
            pltpu.SemaphoreType.DMA((2, n)),
            pltpu.SemaphoreType.DMA((max(n_next, 1),)),
        ],
        compiler_params=params(8),
        cost_estimate=cost(2 * n * cap * width, 4 * n * cap * width),
        name="dots",
    )(in_hbm(eo), *map(in_hbm, chunks))


def last_dots_kernel(n_width, groups, last, side, gate_ref, eo_ref, *refs):
    chunk_refs, early_refs, out_ref = refs[:side], refs[side:-1], refs[-1]
    place = here()

    def put(src, row):
        both = jnp.concatenate([row, gate_ref[pl.ds(src, 1), :]], axis=1)
        for w in range(n_width):
            out_ref[src * n_width + w] = both

    for (batch, dests), early in zip(groups, early_refs):
        for at, src in enumerate(cells_of(batch, dests, place)):
            put(src, early[at : at + 1, :])
    for at, src in enumerate(cells_of(last, range(side), place)):
        put(src, row_dots(chunk_refs[at], eo_ref.at[at]))


def tail_kernel(n_expert, n_width, per_device, got_ref, parts_ref, ids_ref, slots_ref, tok_ref, lg_ref, router_ref):
    top, tok = ids_ref.shape
    rows = []
    for e in range(n_expert):
        row = got_ref[e * n_width]
        for w in range(1, n_width):
            row = row + got_ref[e * n_width + w]
        rows.append(row)
    cap = got_ref.shape[2] // 2
    dots = jnp.concatenate(rows, axis=0)[:, :cap]
    high = dots.astype(bf16)
    low = (dots - high.astype(f32)).astype(bf16)
    both = jnp.concatenate([high, low], axis=0)
    ids, slots = ids_ref[...], slots_ref[...]
    dev = ids // per_device
    slot_rows = lax.broadcasted_iota(i32, (cap, tok), 0)
    dev_rows = lax.broadcasted_iota(i32, (n_expert, tok), 0)
    out = []
    for k in range(top):
        table = jnp.where(slot_rows == slots[k : k + 1], 1.0, 0.0).astype(bf16)
        found = jnp.dot(both, table, preferred_element_type=f32)
        found = found[:n_expert] + found[n_expert:]
        out.append(jnp.sum(jnp.where(dev_rows == dev[k : k + 1], found, 0.0), axis=0, keepdims=True))
    gate_grads = jnp.concatenate(out, axis=0)
    picked, totals = gates_of(parts_ref[...])
    weighted = jnp.sum(gate_grads * picked, axis=0, keepdims=True) / totals
    local = route_scale / totals * (gate_grads - weighted) * picked * (1.0 - picked)
    experts = lax.broadcasted_iota(i32, (lg_ref.shape[0], tok), 0)
    grads = jnp.zeros(lg_ref.shape, f32)
    for k in range(top):
        grads = grads + jnp.where(experts == ids[k : k + 1], local[k : k + 1], 0.0)
    grads = grads.astype(bf16)
    lg_ref[...] = grads
    router_ref[...] = jnp.dot(grads, tok_ref[...], preferred_element_type=f32).astype(bf16)


def scale_kernel(n_width, batches, cap, side, got_ref, lg_ref, w_ref, *refs):
    chunk_refs, (out_ref, input_ref, held, stage, in_sem, sem) = refs[:-6], refs[-6:]
    place = here()
    rows = fetch_chunks(chunk_refs, held, in_sem, cap)
    copies = []
    cells = sum([cells_of(batch, range(side), place) for batch in batches], [])
    for at, src in enumerate(cells):
        gate = jnp.broadcast_to(got_ref[src * n_width][:, cap:], (128, cap)).T
        rows[at].wait()
        for lane in range(0, held.shape[2], 128):
            part = held[at, :, lane : lane + 128].astype(f32)
            stage[at, :, lane : lane + 128] = (part * gate).astype(bf16)
        to = out_ref.at[pl.ds(pl.multiple_of(src * cap, cap), cap), :]
        copies.append(pltpu.make_async_copy(stage.at[at], to, sem.at[at]))
        copies[-1].start()
    input_ref[...] = lax.dot_general(
        lg_ref[...], w_ref[...], (((0,), (1,)), ((), ())), preferred_element_type=f32
    ).astype(bf16)
    for copy in copies:
        copy.wait()


def body(tokens_in, out_grad, router_weight, expert_out, expert_ids, slot_ids):
    n_expert, n_width = lax.axis_size("expert"), lax.axis_size("width")
    side = int(round(n_expert**0.5))
    tok, width = out_grad.shape
    top = expert_ids.shape[1]
    experts = router_weight.shape[1]
    per_device = experts // n_expert
    cap = tok * top // n_expert

    def send(x, shift, second):
        return lax.ppermute(x, AXES, line_shift(n_expert, n_width, shift, second))

    ids, slots = expert_ids.T, slot_ids.T
    half = tok // 2
    first, last = pl.pallas_call(
        functools.partial(pack_kernel, per_device),
        out_shape=[
            jax.ShapeDtypeStruct((half, width), bf16),
            jax.ShapeDtypeStruct((tok - half + top, width), bf16),
        ],
        in_specs=[HBM] * 3,
        out_specs=[VMEM] * 2,
        scratch_shapes=[
            pltpu.VMEM((top, tok), i32),
            pltpu.VMEM((top, tok), i32),
            pltpu.SemaphoreType.DMA((4,)),
        ],
        compiler_params=params(4),
        cost_estimate=cost(0, 4 * tok * width),
        name="pack",
    )(in_hbm(out_grad), in_hbm(ids), in_hbm(slots))
    up_first = send(first, 1, False)
    down_last = send(last, side - 1, False)
    up_last = send(last, 1, False)
    down_first = send(first, side - 1, False)
    far = [send(up_first, 1, False), send(down_last, side - 1, False)]
    sources = {0: [first, last], 1: [up_first, up_last], side - 1: [down_first, down_last], 2: far}
    batches = [[0, 1, side - 1], [2]]

    sent_parts = front(ids, tokens_in, router_weight, n_width)
    parts = lax.all_to_all(sent_parts, "width", 0, 0, tiled=True)

    landed = []
    for b, batch in enumerate(batches):
        group = [None] * side
        for dests in PARTS[b]:
            chunks = compact([sources[s] for s in batch], tok, cap, dests)
            for d, chunk in zip(dests, chunks):
                group[d] = chunk if d == 0 else send(chunk, d, True)
        landed.append(group)

    gates = pl.pallas_call(
        functools.partial(gate_kernel, per_device),
        out_shape=jax.ShapeDtypeStruct((n_expert, cap), f32),
        in_specs=[VMEM] * 3,
        out_specs=VMEM,
        compiler_params=params(4),
        cost_estimate=cost(2 * top * n_expert * cap * tok, 4 * n_width * top * tok),
        name="gates",
    )(parts, ids, slots)

    early, groups, ahead = [], [], None
    for b, batch in enumerate(batches[:-1]):
        for dests in DOTS:
            ahead_cells = (batches[-1], range(side)) if ahead is None else ()
            outs = row_dots_call(batch, dests, ahead_cells, expert_out, [landed[b][d] for d in dests], cap)
            ahead = outs[1] if ahead is None else ahead
            early.append(outs[0])
            groups.append((batch, dests))
    sent = pl.pallas_call(
        functools.partial(last_dots_kernel, n_width, groups, batches[-1], side),
        out_shape=jax.ShapeDtypeStruct((n_expert * n_width, 1, 2 * cap), f32),
        in_specs=[VMEM] * (2 + side + len(early)),
        out_specs=VMEM,
        compiler_params=params(6),
        cost_estimate=cost(2 * side * cap * width, 4 * side * cap * width),
        name="last_dots",
    )(gates, ahead, *landed[-1], *early)
    got = lax.all_to_all(sent, AXES, 0, 0, tiled=True)

    logit_grads, router_part = pl.pallas_call(
        functools.partial(tail_kernel, n_expert, n_width, per_device),
        out_shape=[
            jax.ShapeDtypeStruct((experts, tok), bf16),
            jax.ShapeDtypeStruct((experts, width), bf16),
        ],
        in_specs=[VMEM] * 5,
        out_specs=[VMEM] * 2,
        compiler_params=params(8),
        cost_estimate=cost(2 * tok * width * experts, 2 * tok * width),
        name="tail",
    )(got, parts, ids, slots, tokens_in)
    blocks = lax.all_to_all(router_part.reshape(n_expert, per_device, width), "expert", 0, 0, tiled=True)
    flat = sum(landed, [])
    expert_grad, input_grad = pl.pallas_call(
        functools.partial(scale_kernel, n_width, batches, cap, side),
        out_shape=[
            jax.ShapeDtypeStruct(expert_out.shape, bf16),
            jax.ShapeDtypeStruct((tok, width), bf16),
        ],
        in_specs=[VMEM] * 3 + [HBM] * len(flat),
        out_specs=[HBM, VMEM],
        scratch_shapes=[
            pltpu.VMEM((n_expert, cap, width), bf16),
            pltpu.VMEM((n_expert, cap, width), bf16),
            pltpu.SemaphoreType.DMA((n_expert,)),
            pltpu.SemaphoreType.DMA((n_expert,)),
        ],
        compiler_params=params(16),
        cost_estimate=cost(2 * tok * width * experts, 4 * n_expert * cap * width),
        name="scale",
    )(got, logit_grads, router_weight, *map(in_hbm, flat))
    router_grad = jnp.sum(blocks.astype(f32), axis=0).T
    return (expert_grad, router_grad, input_grad)


def solution(mesh):
    return jax.shard_map(
        body,
        mesh=mesh,
        in_specs=(
            P("expert", "width"),
            P("expert", "width"),
            P("width", None),
            P("expert", "width"),
            P("expert", None),
            P("expert", None),
        ),
        out_specs=(P("expert", "width"), P("width", "expert"), P("expert", "width")),
        check_vma=False,
    )
```

```python
import functools

import jax
import jax.numpy as jnp
from jax import lax
from jax.experimental import pallas as pl
from jax.experimental.pallas import tpu as pltpu
from jax.sharding import PartitionSpec as P


route_scale = 2.5
AXES = ("expert", "width")
f32, bf16, i32 = jnp.float32, jnp.bfloat16, jnp.int32
DIRECT = False
PARTS = (((2,), (1,), (3,), (0,)), ((2,), (1, 3), (0,)))
DOTS = ((0,), (2,), (1, 3))
VMEM = pl.BlockSpec(memory_space=pltpu.VMEM)
SMEM = pl.BlockSpec(memory_space=pltpu.SMEM)
ANY = pl.BlockSpec(memory_space=pl.ANY)
HBM = pl.BlockSpec(memory_space=pltpu.HBM)


def params(mib):
    return pltpu.CompilerParams(vmem_limit_bytes=mib * 1024 * 1024)


def cost(flops, moved):
    return pl.CostEstimate(flops=flops, bytes_accessed=moved, transcendentals=0)


def line_shift(n_expert, n_width, shift, second):
    side = int(round(n_expert**0.5))
    pairs = []
    for e in range(n_expert):
        y, z = e // side, e % side
        for w in range(n_width):
            if (w % 2 == 0) != second:
                to = ((y + shift) % side) * side + z
            else:
                to = y * side + (z + shift) % side
            pairs.append((e * n_width + w, to * n_width + w))
    return pairs


def here():
    n_expert = lax.axis_size("expert")
    side = int(round(n_expert**0.5))
    me = lax.axis_index("expert")
    return side, lax.div(me, side), lax.rem(me, side), lax.rem(lax.axis_index("width"), 2)


def cell(place, along, across):
    side, y, z, core = place
    along, across = along % side, across % side
    first = lax.rem(y + along, side) * side + lax.rem(z + across, side)
    second = lax.rem(y + across, side) * side + lax.rem(z + along, side)
    return jnp.where(core == 0, first, second)


def in_hbm(x):
    return pltpu.with_memory_space_constraint(x, pltpu.HBM)


def pack_kernel(per_device, x_ref, ids_ref, slots_ref, first_ref, last_ref, held_ids, held_slots, sem):
    tok, width = x_ref.shape
    top, half = ids_ref.shape[0], first_ref.shape[0]
    copies = [
        pltpu.make_async_copy(ids_ref, held_ids, sem.at[0]),
        pltpu.make_async_copy(slots_ref, held_slots, sem.at[1]),
        pltpu.make_async_copy(x_ref.at[pl.ds(0, half), :], first_ref, sem.at[2]),
        pltpu.make_async_copy(x_ref.at[pl.ds(half, tok - half), :], last_ref.at[pl.ds(0, tok - half), :], sem.at[3]),
    ]
    for copy in copies:
        copy.start()
    copies[0].wait()
    copies[1].wait()
    dev = (held_ids[...] // per_device).astype(f32)
    slots = held_slots[...].astype(f32)
    rest = jnp.zeros((top, width - 2 * tok), f32)
    last_ref[tok - half :, :] = jnp.concatenate([dev, slots, rest], axis=1).astype(bf16)
    copies[2].wait()
    copies[3].wait()


def compact_kernel(parts, tok, cap, dests, direct, *refs):
    n_in, n_dest = sum(parts), len(dests)
    x_refs = refs[:n_in]
    out_refs = refs[n_in : n_in + n_dest]
    place = here()
    copies = []
    for out, d in enumerate(dests):
        at = 0
        for j, count in enumerate(parts):
            mine_refs = x_refs[at : at + count]
            at += count
            last = mine_refs[-1].shape[0]
            top = sum(ref.shape[0] for ref in mine_refs) - tok
            info = mine_refs[-1][last - top :, :].astype(f32)
            dev, slots = info[:, :tok], info[:, tok : 2 * tok]
            mine = dev == cell(place, 0, d).astype(f32)
            slot = jnp.sum(jnp.where(mine, slots + 1.0, 0.0), axis=0, keepdims=True).astype(i32) - 1
            got, first = None, 0
            for ref in mine_refs:
                rows = min(ref.shape[0], tok - first)
                want = lax.broadcasted_iota(i32, (cap, rows), 0)
                table = jnp.where(want == slot[:, first : first + rows], 1.0, 0.0).astype(bf16)
                term = jnp.dot(table, ref[:rows, :], preferred_element_type=f32)
                got = term if got is None else got + term
                first += rows
            if direct:
                out_refs[out][j * cap : (j + 1) * cap, :] = got.astype(bf16)
            else:
                stage, sem = refs[-2:]
                stage[out, j] = got.astype(bf16)
                to = out_refs[out].at[pl.ds(j * cap, cap), :]
                copies.append(pltpu.make_async_copy(stage.at[out, j], to, sem.at[out, j]))
                copies[-1].start()
    for copy in copies:
        copy.wait()


def compact(sources, tok, cap, dests):
    n_src, width, n_dest = len(sources), sources[0][0].shape[1], len(dests)
    xs = sum(sources, [])
    direct = DIRECT and 0 not in dests
    shape = (n_src * cap, width)
    scratch = [pltpu.VMEM((n_dest, n_src, cap, width), bf16), pltpu.SemaphoreType.DMA((n_dest, n_src))]
    return pl.pallas_call(
        functools.partial(compact_kernel, [len(x) for x in sources], tok, cap, dests, direct),
        out_shape=[jax.ShapeDtypeStruct(shape, bf16) if direct else pltpu.HBM(shape, bf16)] * n_dest,
        in_specs=[VMEM] * len(xs),
        out_specs=[VMEM if direct else HBM] * n_dest,
        scratch_shapes=[] if direct else scratch,
        compiler_params=params(8),
        cost_estimate=cost(2 * n_src * n_dest * cap * tok * width, n_src * tok * width * 6),
        name="compact",
    )(*xs)


def picked_kernel(ids_ref, tok_ref, w_ref, out_ref, ids, toks, weights, sem):
    copies = [
        pltpu.make_async_copy(w_ref, weights, sem.at[0]),
        pltpu.make_async_copy(tok_ref, toks, sem.at[1]),
        pltpu.make_async_copy(ids_ref, ids, sem.at[2]),
    ]
    for copy in copies:
        copy.start()
    for copy in copies:
        copy.wait()
    logits = lax.dot_general(
        weights[...], toks[...], (((0,), (1,)), ((), ())), preferred_element_type=f32
    )
    experts = lax.broadcasted_iota(i32, logits.shape, 0)
    rows = []
    for k in range(ids.shape[0]):
        hit = experts == ids[k : k + 1, :]
        rows.append(jnp.sum(jnp.where(hit, logits, 0.0), axis=0, keepdims=True))
    picked = jnp.concatenate(rows, axis=0)
    for w in range(out_ref.shape[0]):
        out_ref[w] = picked


def front(ids, tokens_in, router_weight, n_width):
    (top, tok), width, experts = ids.shape, tokens_in.shape[1], router_weight.shape[1]
    return pl.pallas_call(
        picked_kernel,
        out_shape=jax.ShapeDtypeStruct((n_width, top, tok), f32),
        in_specs=[HBM] * 3,
        out_specs=VMEM,
        scratch_shapes=[
            pltpu.VMEM((top, tok), i32),
            pltpu.VMEM((tok, width), bf16),
            pltpu.VMEM((width, experts), bf16),
            pltpu.SemaphoreType.DMA((3,)),
        ],
        compiler_params=params(6),
        cost_estimate=cost(2 * tok * width * experts, 2 * tok * width),
        name="picked",
    )(in_hbm(ids), in_hbm(tokens_in), in_hbm(router_weight))


def gates_of(parts):
    logits = jnp.sum(parts, axis=0)
    picked = 1.0 / (1.0 + jnp.exp(-logits))
    totals = jnp.sum(picked, axis=0, keepdims=True)
    return picked, totals


def gate_kernel(per_device, parts_ref, ids_ref, slots_ref, out_ref):
    picked, totals = gates_of(parts_ref[...])
    gates = (route_scale * picked / totals).astype(bf16).astype(f32)
    top, tok = ids_ref.shape
    n_expert, cap = out_ref.shape
    dev, slots = ids_ref[...] // per_device, slots_ref[...]
    dev_rows = lax.broadcasted_iota(i32, (n_expert, tok), 0)
    slot_rows = lax.broadcasted_iota(i32, (cap, tok), 0)
    total = jnp.zeros((n_expert, cap), f32)
    for k in range(top):
        left = jnp.where(dev_rows == dev[k : k + 1], gates[k : k + 1], 0.0).astype(bf16)
        right = jnp.where(slot_rows == slots[k : k + 1], 1.0, 0.0).astype(bf16)
        total = total + lax.dot_general(left, right, (((1,), (1,)), ((), ())), preferred_element_type=f32)
    out_ref[...] = total


def row_dots(chunk, other):
    total = None
    for at in range(0, chunk.shape[1], 128):
        term = chunk[:, at : at + 128].astype(f32) * other[:, at : at + 128].astype(f32)
        total = term if total is None else total + term
    return jnp.sum(total.T, axis=0, keepdims=True)


def fetch(eo_ref, stage, sem, cells, cap):
    copies = []
    for at, src in enumerate(cells):
        rows = eo_ref.at[pl.ds(pl.multiple_of(src * cap, cap), cap), :]
        copies.append(pltpu.make_async_copy(rows, stage.at[at], sem.at[at]))
        copies[-1].start()
    return copies


def fetch_chunks(chunk_refs, stage, sem, cap, first=0):
    copies, at = [], first
    for chunk_ref in chunk_refs:
        for j in range(chunk_ref.shape[0] // cap):
            copies.append(pltpu.make_async_copy(chunk_ref.at[pl.ds(j * cap, cap), :], stage.at[at], sem.at[at]))
            copies[-1].start()
            at += 1
    return copies


def cells_of(batch, dests, place):
    return [cell(place, -s, -d) for d in dests for s in batch]


def dots_kernel(batch, dests, cap, ahead_cells, eo_ref, *refs):
    chunk_refs = refs[: len(dests)]
    out_refs, (held, stage, sem, next_sem) = refs[len(dests) : -4], refs[-4:]
    place = here()
    rows = fetch_chunks(chunk_refs, held, sem.at[0], cap)
    others = fetch(eo_ref, stage, sem.at[1], cells_of(batch, dests, place), cap)
    ahead = fetch(eo_ref, out_refs[1], next_sem, cells_of(*ahead_cells, place), cap) if ahead_cells else []
    for at in range(len(rows)):
        rows[at].wait()
        others[at].wait()
        out_refs[0][at : at + 1, :] = row_dots(held.at[at], stage.at[at])
    for copy in ahead:
        copy.wait()


def row_dots_call(batch, dests, ahead_cells, eo, chunks, cap):
    n, width = len(batch) * len(dests), chunks[0].shape[1]
    n_next = len(ahead_cells[0]) * len(ahead_cells[1]) if ahead_cells else 0
    outs = [jax.ShapeDtypeStruct((n, cap), f32)]
    if n_next:
        outs.append(pltpu.VMEM((n_next, cap, width), bf16))
    return pl.pallas_call(
        functools.partial(dots_kernel, batch, dests, cap, ahead_cells),
        out_shape=outs,
        in_specs=[HBM] * (1 + len(dests)),
        out_specs=[VMEM] * len(outs),
        scratch_shapes=[
            pltpu.VMEM((n, cap, width), bf16),
            pltpu.VMEM((n, cap, width), bf16),
            pltpu.SemaphoreType.DMA((2, n)),
            pltpu.SemaphoreType.DMA((max(n_next, 1),)),
        ],
        compiler_params=params(8),
        cost_estimate=cost(2 * n * cap * width, 4 * n * cap * width),
        name="dots",
    )(in_hbm(eo), *map(in_hbm, chunks))


def last_dots_kernel(n_width, groups, last, side, gate_ref, eo_ref, *refs):
    chunk_refs, early_refs, out_ref = refs[:side], refs[side:-1], refs[-1]
    place = here()

    def put(src, row):
        both = jnp.concatenate([row, gate_ref[pl.ds(src, 1), :]], axis=1)
        for w in range(n_width):
            out_ref[src * n_width + w] = both

    for (batch, dests), early in zip(groups, early_refs):
        for at, src in enumerate(cells_of(batch, dests, place)):
            put(src, early[at : at + 1, :])
    for at, src in enumerate(cells_of(last, range(side), place)):
        put(src, row_dots(chunk_refs[at], eo_ref.at[at]))


def tail_kernel(n_expert, n_width, per_device, got_ref, parts_ref, ids_ref, slots_ref, tok_ref, *refs):
    lg_ref, router_ref, stage, sem = refs
    top, tok = ids_ref.shape
    rows = []
    for e in range(n_expert):
        row = got_ref[e * n_width]
        for w in range(1, n_width):
            row = row + got_ref[e * n_width + w]
        rows.append(row)
    cap = got_ref.shape[2] // 2
    dots = jnp.concatenate(rows, axis=0)[:, :cap]
    high = dots.astype(bf16)
    low = (dots - high.astype(f32)).astype(bf16)
    both = jnp.concatenate([high, low], axis=0)
    ids, slots = ids_ref[...], slots_ref[...]
    dev = ids // per_device
    slot_rows = lax.broadcasted_iota(i32, (cap, tok), 0)
    dev_rows = lax.broadcasted_iota(i32, (n_expert, tok), 0)
    tables = [jnp.where(slot_rows == slots[k : k + 1], 1.0, 0.0).astype(bf16) for k in range(top)]
    found = jnp.dot(both, jnp.concatenate(tables, axis=1), preferred_element_type=f32)
    found = found[:n_expert] + found[n_expert:]
    out = []
    for k in range(top):
        mine = jnp.where(dev_rows == dev[k : k + 1], found[:, k * tok : (k + 1) * tok], 0.0)
        out.append(jnp.sum(mine, axis=0, keepdims=True))
    gate_grads = jnp.concatenate(out, axis=0)
    picked, totals = gates_of(parts_ref[...])
    weighted = jnp.sum(gate_grads * picked, axis=0, keepdims=True) / totals
    local = route_scale / totals * (gate_grads - weighted) * picked * (1.0 - picked)
    experts = lax.broadcasted_iota(i32, (lg_ref.shape[0], tok), 0)
    grads = jnp.zeros(lg_ref.shape, f32)
    for k in range(top):
        grads = grads + jnp.where(experts == ids[k : k + 1], local[k : k + 1], 0.0)
    grads = grads.astype(bf16)
    lg_ref[...] = grads
    copies = []
    rows = grads.shape[0] // 2
    for at in range(2):
        part = grads[at * rows : (at + 1) * rows]
        stage[at] = jnp.dot(part, tok_ref[...], preferred_element_type=f32).astype(bf16)
        copies.append(pltpu.make_async_copy(stage.at[at], router_ref.at[pl.ds(at * rows, rows), :], sem.at[at]))
        copies[-1].start()
    for copy in copies:
        copy.wait()


def scale_kernel(n_width, batches, cap, side, got_ref, lg_ref, w_ref, *refs):
    chunk_refs, (out_ref, input_ref, held, stage, in_sem, sem) = refs[:-6], refs[-6:]
    place = here()
    rows = fetch_chunks(chunk_refs, held, in_sem, cap)
    copies = []
    cells = sum([cells_of(batch, range(side), place) for batch in batches], [])
    for at, src in enumerate(cells):
        gate = jnp.broadcast_to(got_ref[src * n_width][:, cap:], (128, cap)).T
        rows[at].wait()
        for lane in range(0, held.shape[2], 128):
            part = held[at, :, lane : lane + 128].astype(f32)
            stage[at, :, lane : lane + 128] = (part * gate).astype(bf16)
        to = out_ref.at[pl.ds(pl.multiple_of(src * cap, cap), cap), :]
        copies.append(pltpu.make_async_copy(stage.at[at], to, sem.at[at]))
        copies[-1].start()
    input_ref[...] = lax.dot_general(
        lg_ref[...], w_ref[...], (((0,), (1,)), ((), ())), preferred_element_type=f32
    ).astype(bf16)
    for copy in copies:
        copy.wait()


def body(tokens_in, out_grad, router_weight, expert_out, expert_ids, slot_ids):
    n_expert, n_width = lax.axis_size("expert"), lax.axis_size("width")
    side = int(round(n_expert**0.5))
    tok, width = out_grad.shape
    top = expert_ids.shape[1]
    experts = router_weight.shape[1]
    per_device = experts // n_expert
    cap = tok * top // n_expert

    def send(x, shift, second):
        return lax.ppermute(x, AXES, line_shift(n_expert, n_width, shift, second))

    ids, slots = expert_ids.T, slot_ids.T
    half = tok // 2
    first, last = pl.pallas_call(
        functools.partial(pack_kernel, per_device),
        out_shape=[
            jax.ShapeDtypeStruct((half, width), bf16),
            jax.ShapeDtypeStruct((tok - half + top, width), bf16),
        ],
        in_specs=[HBM] * 3,
        out_specs=[VMEM] * 2,
        scratch_shapes=[
            pltpu.VMEM((top, tok), i32),
            pltpu.VMEM((top, tok), i32),
            pltpu.SemaphoreType.DMA((4,)),
        ],
        compiler_params=params(4),
        cost_estimate=cost(0, 4 * tok * width),
        name="pack",
    )(in_hbm(out_grad), in_hbm(ids), in_hbm(slots))
    up_first = send(first, 1, False)
    down_last = send(last, side - 1, False)
    up_last = send(last, 1, False)
    down_first = send(first, side - 1, False)
    far = [send(up_first, 1, False), send(down_last, side - 1, False)]
    sources = {0: [first, last], 1: [up_first, up_last], side - 1: [down_first, down_last], 2: far}
    batches = [[0, 1, side - 1], [2]]

    sent_parts = front(ids, tokens_in, router_weight, n_width)
    parts = lax.all_to_all(sent_parts, "width", 0, 0, tiled=True)

    landed = []
    for b, batch in enumerate(batches):
        group = [None] * side
        for dests in PARTS[b]:
            chunks = compact([sources[s] for s in batch], tok, cap, dests)
            for d, chunk in zip(dests, chunks):
                group[d] = chunk if d == 0 else send(chunk, d, True)
        landed.append(group)

    gates = pl.pallas_call(
        functools.partial(gate_kernel, per_device),
        out_shape=jax.ShapeDtypeStruct((n_expert, cap), f32),
        in_specs=[VMEM] * 3,
        out_specs=VMEM,
        compiler_params=params(4),
        cost_estimate=cost(2 * top * n_expert * cap * tok, 4 * n_width * top * tok),
        name="gates",
    )(parts, ids, slots)

    early, groups, ahead = [], [], None
    for b, batch in enumerate(batches[:-1]):
        for dests in DOTS:
            ahead_cells = (batches[-1], range(side)) if ahead is None else ()
            outs = row_dots_call(batch, dests, ahead_cells, expert_out, [landed[b][d] for d in dests], cap)
            ahead = outs[1] if ahead is None else ahead
            early.append(outs[0])
            groups.append((batch, dests))
    sent = pl.pallas_call(
        functools.partial(last_dots_kernel, n_width, groups, batches[-1], side),
        out_shape=jax.ShapeDtypeStruct((n_expert * n_width, 1, 2 * cap), f32),
        in_specs=[VMEM] * (2 + side + len(early)),
        out_specs=VMEM,
        compiler_params=params(6),
        cost_estimate=cost(2 * side * cap * width, 4 * side * cap * width),
        name="last_dots",
    )(gates, ahead, *landed[-1], *early)
    got = lax.all_to_all(sent, AXES, 0, 0, tiled=True)

    logit_grads, router_part = pl.pallas_call(
        functools.partial(tail_kernel, n_expert, n_width, per_device),
        out_shape=[
            jax.ShapeDtypeStruct((experts, tok), bf16),
            pltpu.HBM((experts, width), bf16),
        ],
        in_specs=[VMEM] * 5,
        out_specs=[VMEM, HBM],
        scratch_shapes=[
            pltpu.VMEM((2, experts // 2, width), bf16),
            pltpu.SemaphoreType.DMA((2,)),
        ],
        compiler_params=params(8),
        cost_estimate=cost(2 * tok * width * experts, 2 * tok * width),
        name="tail",
    )(got, parts, ids, slots, tokens_in)
    blocks = lax.all_to_all(router_part.reshape(n_expert, per_device, width), "expert", 0, 0, tiled=True)
    flat = sum(landed, [])
    expert_grad, input_grad = pl.pallas_call(
        functools.partial(scale_kernel, n_width, batches, cap, side),
        out_shape=[
            jax.ShapeDtypeStruct(expert_out.shape, bf16),
            jax.ShapeDtypeStruct((tok, width), bf16),
        ],
        in_specs=[VMEM] * 3 + [HBM] * len(flat),
        out_specs=[HBM, VMEM],
        scratch_shapes=[
            pltpu.VMEM((n_expert, cap, width), bf16),
            pltpu.VMEM((n_expert, cap, width), bf16),
            pltpu.SemaphoreType.DMA((n_expert,)),
            pltpu.SemaphoreType.DMA((n_expert,)),
        ],
        compiler_params=params(16),
        cost_estimate=cost(2 * tok * width * experts, 4 * n_expert * cap * width),
        name="scale",
    )(got, logit_grads, router_weight, *map(in_hbm, flat))
    router_grad = jnp.sum(blocks.astype(f32), axis=0).T
    return (expert_grad, router_grad, input_grad)


def solution(mesh):
    return jax.shard_map(
        body,
        mesh=mesh,
        in_specs=(
            P("expert", "width"),
            P("expert", "width"),
            P("width", None),
            P("expert", "width"),
            P("expert", None),
            P("expert", None),
        ),
        out_specs=(P("expert", "width"), P("width", "expert"), P("expert", "width")),
        check_vma=False,
    )
```
